32 devices in a mesh: ctx: 8 (over z, y), head: 4 (over x, core).
Axes of the slice: x: 2, y: 2, z: 4, core: 2. Of those that a mesh axis runs over, the one named last changes fastest.
Arguments:
- queries: bfloat16 [2048, 5120], P('ctx', 'head'), parts along dimension 1, may hold values from -6 to 6
- query_tangents: bfloat16 [2048, 5120], P('ctx', 'head'), parts along dimension 1, may hold values from -6 to 6
- keys: bfloat16 [2048, 5120], P('ctx', 'head'), parts along dimension 1, may hold values from -6 to 6
- key_tangents: bfloat16 [2048, 5120], P('ctx', 'head'), parts along dimension 1, may hold values from -6 to 6
- values: bfloat16 [2048, 5120], P('ctx', 'head'), parts along dimension 1, may hold values from -6 to 6
- value_tangents: bfloat16 [2048, 5120], P('ctx', 'head'), parts along dimension 1, may hold values from -6 to 6
- selection: int32 [16, 14], P('ctx'), may hold values from 0 to 1, as said below
Outputs:
- attention_out: bfloat16 [2048, 5120], P('ctx', 'head'), parts along dimension 1
- attention_tangent: bfloat16 [2048, 5120], P('ctx', 'head'), parts along dimension 1
The draws below stay inside these ranges and needn't reach their ends.
There are 4 independent parts, one for each index of `head`. The reference program is written for one: setup_inputs(seed, part) draws one part's arguments, and reference() takes and returns one part's arrays. A program takes and returns all parts, laid end to end along the dimension named above; an argument that names none is the same for every part. Nothing has to cross between parts.
Inputs may be any that keep to these rules, and one draw needn't show every extreme that they name: `selection`: column 6 + b mod 2 of row b, the query block's own block, is always 1.
All inputs are finite; a program needn't handle non-finite values.
Results may differ from the reference program's by a relative error of at most 0.012.
Values may be sent and summed in bfloat16 or wider, within the bound.
A program may use at most 128 MiB of HBM per device.

```python
import jax
import jax.numpy as jnp
from jax import lax

HEADS = 10
HEAD_DIM = 128
BLK = 128
REACH = 3
TOK_DEV = 256
TOKENS = 2048
BPD = 2
QBLOCKS = 16
WIN = 14
N_CTX = 8


def draw_queries(key, part):
    sample_field = jax.random.normal(jax.random.fold_in(key, 21), (TOKENS, HEADS * HEAD_DIM), jnp.float32) * 1.4
    return jnp.clip(sample_field, -6.0, 6.0).astype(jnp.bfloat16)


def draw_keys(key, part):
    sample_field = jax.random.normal(jax.random.fold_in(key, 22), (TOKENS, HEADS * HEAD_DIM), jnp.float32) * 1.4
    return jnp.clip(sample_field, -6.0, 6.0).astype(jnp.bfloat16)


def draw_selection(key, part):
    levels = jax.random.randint(jax.random.fold_in(key, 31), (N_CTX,), 0, 8)
    dice_rolls = jax.random.randint(jax.random.fold_in(key, 32), (QBLOCKS, WIN), 0, 16)
    blocks = jnp.arange(QBLOCKS, dtype=jnp.int32)
    owners = blocks // BPD
    limits = 2 + 2 * jnp.take(levels, owners)
    chosen = dice_rolls < limits[:, None]
    columns = jnp.arange(WIN, dtype=jnp.int32)
    itself = columns[None, :] == (REACH * BPD + blocks % BPD)[:, None]
    return jnp.where(chosen | itself, 1, 0).astype(jnp.int32)


def block_levels(own_key, shape, split, low, top_value):
    def one(axis_at, parts):
        heights = jax.random.uniform(jax.random.fold_in(jax.random.fold_in(own_key, 6), axis_at), (parts,), jnp.float32, low / len(split), top_value / len(split))
        return jnp.repeat(jnp.exp(heights), shape[axis_at] // parts).reshape((-1,) + (1,) * (len(shape) - axis_at - 1))

    level = one(*split[0])
    for cut in split[1:]:
        level = level * one(*cut)
    return level


def noise(stream_key, dims, width, bound, cuts=(), kind=jnp.bfloat16):
    values = jax.random.normal(stream_key, dims, jnp.float32) * width
    if len(cuts) > 0:
        values = block_levels(stream_key, dims, cuts, -0.22, 0.18) * values
    return jnp.clip(values, min=-bound, max=bound).astype(kind)


def setup_inputs(seed: int = 0, part: int = 0) -> dict:
    key_of = jax.random.split(jax.random.key(seed), 8)
    part_splits = jax.random.split(jax.random.fold_in(key_of[7], part), 8)
    return {
        "queries": draw_queries(jax.random.fold_in(jax.random.fold_in(key_of[7], part), 71), part),
        "query_tangents": noise(part_splits[1], (TOKENS, HEADS * HEAD_DIM), 1.0, 6.0, ((0, 8),)),
        "keys": draw_keys(jax.random.fold_in(jax.random.fold_in(key_of[7], part), 71), part),
        "key_tangents": noise(part_splits[3], (TOKENS, HEADS * HEAD_DIM), 1.0, 6.0, ((0, 8),)),
        "values": noise(part_splits[4], (TOKENS, HEADS * HEAD_DIM), 1.0, 6.0, ((0, 8),)),
        "value_tangents": noise(part_splits[5], (TOKENS, HEADS * HEAD_DIM), 1.0, 6.0, ((0, 8),)),
        "selection": draw_selection(jax.random.fold_in(key_of[7], 71), part),
    }


big_negative = -1.0e30


def reference(queries, query_tangents, keys, key_tangents, values, value_tangents, selection):
    score_scale = HEAD_DIM ** -0.5
    per_device = TOK_DEV // BLK
    window = (2 * REACH + 1) * per_device
    block_count = TOKENS // BLK

    def split_blocks(flat_array):
        return flat_array.reshape(block_count, BLK, HEADS, HEAD_DIM)

    query_blocks = split_blocks(queries)
    query_tangent_blocks = split_blocks(query_tangents)
    key_blocks = split_blocks(keys)
    key_tangent_blocks = split_blocks(key_tangents)
    value_blocks = split_blocks(values)
    value_tangent_blocks = split_blocks(value_tangents)
    columns = jnp.arange(window, dtype=jnp.int32)

    def one_block(block_index):
        owner_device = block_index // per_device
        source = ((owner_device + columns // per_device - REACH) % N_CTX) * per_device + columns % per_device
        source = source.astype(jnp.int32)

        def window_of(blocks):
            return jnp.take(blocks, source, axis=0).reshape(window * BLK, HEADS, HEAD_DIM).astype(jnp.float32)

        key_window = window_of(key_blocks)
        key_tangent_window = window_of(key_tangent_blocks)
        value_window = window_of(value_blocks)
        value_tangent_window = window_of(value_tangent_blocks)
        query_block = lax.dynamic_index_in_dim(query_blocks, block_index, 0, keepdims=False).astype(jnp.float32)
        query_tangent = lax.dynamic_index_in_dim(query_tangent_blocks, block_index, 0, keepdims=False).astype(jnp.float32)
        chosen = lax.dynamic_index_in_dim(selection, block_index, 0, keepdims=False) != 0
        key_mask = jnp.repeat(chosen, BLK)[None, None, :]
        scores = jnp.einsum("qhd,khd->qhk", query_block, key_window) * score_scale
        score_tangents = (jnp.einsum("qhd,khd->qhk", query_tangent, key_window)
                          + jnp.einsum("qhd,khd->qhk", query_block, key_tangent_window)) * score_scale
        masked = jnp.where(key_mask, scores, big_negative)
        peak_score = masked.max(axis=2, keepdims=True)
        weights = jnp.where(key_mask, jnp.exp(masked - peak_score), 0.0)
        weighted = weights * score_tangents
        weight_total = weights.sum(axis=2)
        tangent_total = weighted.sum(axis=2)
        rounded_weights = weights.astype(jnp.bfloat16).astype(jnp.float32)
        rounded_tangent = weighted.astype(jnp.bfloat16).astype(jnp.float32)
        mixed_sum = jnp.einsum("qhk,khd->qhd", rounded_weights, value_window)
        mixed_tangent = (jnp.einsum("qhk,khd->qhd", rounded_tangent, value_window)
                         + jnp.einsum("qhk,khd->qhd", rounded_weights, value_tangent_window))
        output = mixed_sum / weight_total[:, :, None]
        tangent = (mixed_tangent - output * tangent_total[:, :, None]) / weight_total[:, :, None]
        return (output.astype(jnp.bfloat16).reshape(BLK, HEADS * HEAD_DIM),
                tangent.astype(jnp.bfloat16).reshape(BLK, HEADS * HEAD_DIM))

    outputs, tangents = lax.map(one_block, jnp.arange(block_count, dtype=jnp.int32))
    return outputs.reshape(TOKENS, HEADS * HEAD_DIM), tangents.reshape(TOKENS, HEADS * HEAD_DIM)
```

```python
import functools

import jax
import jax.numpy as jnp
from jax import lax
from jax.sharding import PartitionSpec as P
from jax.experimental import pallas as pl
from jax.experimental.pallas import tpu as pltpu

HEADS = 10
HEAD_DIM = 128
BLK = 128
REACH = 3


big_negative = -1e30


def from_behind(array, axis, by):
    devices = lax.axis_size(axis)
    return lax.ppermute(array, axis, [(i, (i + by) % devices) for i in range(devices)])


def heads_view(flat_array):
    return flat_array.reshape(flat_array.shape[0], HEADS, HEAD_DIM)


def tile_update(accumulators, query_pieces, key_pieces):
    score_scale = HEAD_DIM ** (-0.5)
    query_block, query_tangent = query_pieces
    key_block, key_tangent, value_block, value_tangent = key_pieces
    running, weight_total, tangent_total, mixed_sum, mixed_tangent = accumulators
    scores = (
        jnp.einsum("qhd,khd->qhk", query_block, key_block, preferred_element_type=jnp.float32)
        * score_scale
    )
    score_tangents = (
        jnp.einsum("qhd,khd->qhk", query_tangent, key_block, preferred_element_type=jnp.float32)
        + jnp.einsum("qhd,khd->qhk", query_block, key_tangent, preferred_element_type=jnp.float32)
    ) * score_scale
    highest = jnp.maximum(running, scores.max(axis=2))
    factor = jnp.exp(running - highest)
    weights = jnp.exp(scores - highest[:, :, None])
    weighted = weights * score_tangents
    weight_total = factor * weight_total + weights.sum(axis=2)
    tangent_total = factor * tangent_total + weighted.sum(axis=2)
    rounded_weights = weights.astype(jnp.bfloat16)
    rounded_tangent = weighted.astype(jnp.bfloat16)
    mixed_sum = factor[:, :, None] * mixed_sum + jnp.einsum(
        "qhk,khd->qhd", rounded_weights, value_block, preferred_element_type=jnp.float32
    )
    mixed_tangent = (
        factor[:, :, None] * mixed_tangent
        + jnp.einsum(
            "qhk,khd->qhd", rounded_tangent, value_block, preferred_element_type=jnp.float32
        )
        + jnp.einsum(
            "qhk,khd->qhd", rounded_weights, value_tangent, preferred_element_type=jnp.float32
        )
    )
    return (highest, weight_total, tangent_total, mixed_sum, mixed_tangent)


def sweep(accumulators, query_pair, chosen_rows, key_pack, column_base):
    per_device = chosen_rows.shape[0]

    def visit(tile_index, carried):
        query_index = tile_index // per_device
        key_index = tile_index % per_device
        picked = chosen_rows[query_index, column_base + key_index] != 0

        def apply(carried_state):
            first_row = query_index * BLK
            pieces = tuple(
                (
                    lax.dynamic_slice_in_dim(full_array, first_row, BLK, 0)
                    for full_array in carried_state
                )
            )
            query_pieces = tuple(
                (
                    lax.dynamic_slice_in_dim(full_array, first_row, BLK, 0)
                    for full_array in query_pair
                )
            )
            key_pieces = tuple(
                (
                    lax.dynamic_slice_in_dim(full_array, key_index * BLK, BLK, 0)
                    for full_array in key_pack
                )
            )
            updated = tile_update(pieces, query_pieces, key_pieces)
            return tuple(
                (
                    lax.dynamic_update_slice_in_dim(full_array, new_piece, first_row, 0)
                    for full_array, new_piece in zip(carried_state, updated)
                )
            )

        return lax.cond(picked, apply, lambda unchanged: unchanged, carried)

    return lax.fori_loop(0, per_device * per_device, visit, tuple(accumulators))


def finish(accumulators):
    running, weight_total, tangent_total, mixed_sum, mixed_tangent = accumulators
    token_count = mixed_sum.shape[0]
    output = mixed_sum / weight_total[:, :, None]
    tangent = (mixed_tangent - output * tangent_total[:, :, None]) / weight_total[:, :, None]
    return (
        output.reshape(token_count, HEADS * HEAD_DIM).astype(jnp.bfloat16),
        tangent.reshape(token_count, HEADS * HEAD_DIM).astype(jnp.bfloat16),
    )


def body(queries, query_tangents, keys, key_tangents, values, value_tangents, selection):
    token_count = queries.shape[0]
    per_device = token_count // BLK
    query_pair = (heads_view(queries), heads_view(query_tangents))
    key_pack = (
        heads_view(keys),
        heads_view(key_tangents),
        heads_view(values),
        heads_view(value_tangents),
    )
    initial = (
        jnp.full((token_count, HEADS), big_negative, jnp.float32),
        jnp.zeros((token_count, HEADS), jnp.float32),
        jnp.zeros((token_count, HEADS), jnp.float32),
        jnp.zeros((token_count, HEADS, HEAD_DIM), jnp.float32),
        jnp.zeros((token_count, HEADS, HEAD_DIM), jnp.float32),
    )
    at_home = sweep(initial, query_pair, selection, key_pack, REACH * per_device)
    accumulators = at_home
    rising = key_pack
    falling = key_pack
    for offset in range(1, REACH + 1):
        rising = from_behind((rising[0], rising[1], rising[2], rising[3]), "ctx", -1)
        accumulators = sweep(
            accumulators, query_pair, selection, rising, (REACH + offset) * per_device
        )
        falling = from_behind((falling[0], falling[1], falling[2], falling[3]), "ctx", 1)
        accumulators = sweep(
            accumulators, query_pair, selection, falling, (REACH - offset) * per_device
        )
    return finish(accumulators)


ORDER = [('M', 0), ('B', 0), ('X', 0), ('M', 1), ('X', 1), ('M', 2), ('X', 2), ('M', 3), ('X', 3), ('X', 4), ('X', 5), ('M', 4), ('M', 5)]
LOG2E = 1.4426950408889634
MESH = pl.DeviceIdType.MESH


def attend(shard, q_slot, n, q_buf, kv_buf, bias_buf, s_buf):
    scale = HEAD_DIM ** (-0.5)
    factor = scale * LOG2E
    width = 2 * REACH + 1
    d = HEAD_DIM
    both = q_buf[q_slot]
    query = q_buf[q_slot, :, d : 2 * d]
    rows = both.shape[0]
    per_device = rows // BLK
    bias = jnp.where(bias_buf[shard] != 0, 0.0, big_negative)
    dims = (((1,), (1,)), ((), ()))
    slots = [lax.rem(shard + n - REACH + j, n) for j in range(width)]
    high = [None] * per_device
    for j in range(width):
        scores = lax.dot_general(
            query, kv_buf[slots[j], :, 0:d], dims, preferred_element_type=jnp.float32
        )
        for r in range(per_device):
            for k in range(per_device):
                column = j * per_device + k
                there = (slice(r * BLK, (r + 1) * BLK), slice(k * BLK, (k + 1) * BLK))
                masked = scores[there] * factor + bias[r : r + 1, column : column + 1]
                s_buf[(j,) + there] = masked
                high[r] = masked if high[r] is None else jnp.maximum(high[r], masked)
    peak = jnp.concatenate([jnp.max(h, axis=1, keepdims=True) for h in high], axis=0)
    total = jnp.zeros((rows, BLK), jnp.float32)
    tangent_total = jnp.zeros((rows, BLK), jnp.float32)
    mixed = jnp.zeros((rows, 2 * d), jnp.float32)
    mixed_tangent = jnp.zeros((rows, d), jnp.float32)
    for j in range(width):
        tangents = lax.dot_general(
            both, kv_buf[slots[j], :, 0 : 2 * d], dims, preferred_element_type=jnp.float32
        )
        weights = jnp.exp2(s_buf[j] - peak)
        weighted = weights * tangents
        for k in range(per_device):
            lanes = slice(k * BLK, (k + 1) * BLK)
            total = total + weights[:, lanes]
            tangent_total = tangent_total + weighted[:, lanes]
        mixed = mixed + jnp.dot(
            weights.astype(jnp.bfloat16),
            kv_buf[slots[j], :, 2 * d : 4 * d],
            preferred_element_type=jnp.float32,
        )
        mixed_tangent = mixed_tangent + jnp.dot(
            weighted.astype(jnp.bfloat16),
            kv_buf[slots[j], :, 2 * d : 3 * d],
            preferred_element_type=jnp.float32,
        )
    inverse = 1.0 / jnp.sum(total, axis=1, keepdims=True)
    tangent_sum = jnp.sum(tangent_total, axis=1, keepdims=True)
    output = mixed[:, 0:d] * inverse
    tangent = (scale * (mixed_tangent - output * tangent_sum) + mixed[:, d : 2 * d]) * inverse
    return output.astype(jnp.bfloat16), tangent.astype(jnp.bfloat16)


def exchange_kernel(
    n, q_ref, qt_ref, k_ref, kt_ref, v_ref, vt_ref, bias_ref, o_ref, ot_ref,
    q_buf, kv_buf, xq_buf, xkv_buf, bias_buf, out_buf, xout_buf, s_buf,
    kv_send, q_send, b_send, o_send, xkv_send, xq_send, xo_send,
    kv_recv, q_recv, b_recv, o_recv, xkv_recv, xq_recv, xo_recv,
):
    d = HEAD_DIM
    half = n // 2
    extra = HEADS - n
    me = lax.axis_index("ctx")
    side = me // half
    place = lax.rem(me, half)
    first_host = half - extra

    def cols(head):
        return pl.ds(pl.multiple_of(head * d, d), d)

    def host(which_side, e):
        return first_host + which_side * extra + e

    barrier = pltpu.get_barrier_semaphore()
    for i in range(1, n):
        pl.semaphore_signal(
            barrier, inc=1, device_id={"ctx": lax.rem(me + i, n)}, device_id_type=MESH
        )
    pl.semaphore_wait(barrier, n - 1)

    def send(src, dst, send_sem, recv_sem, target):
        pltpu.make_async_remote_copy(
            src_ref=src, dst_ref=dst, send_sem=send_sem, recv_sem=recv_sem,
            device_id={"ctx": target}, device_id_type=MESH,
        ).start()

    def wait(ref, sem):
        pltpu.make_async_copy(ref, ref, sem).wait()

    packs = (k_ref, kt_ref, v_ref, vt_ref)
    pair = (qt_ref, q_ref)

    def lane(i):
        return pl.ds(i * d, d)

    def extra_send(ref, i, buf, slot, send_sem, recv_sem, which_side, e):
        target = host(which_side, e)

        @pl.when(target != me)
        def _():
            send(ref.at[:, cols(n + e)], buf.at[slot, :, lane(i)], send_sem, recv_sem.at[slot], target)

        @pl.when(target == me)
        def _():
            pltpu.make_async_copy(ref.at[:, cols(n + e)], buf.at[slot, :, lane(i)], recv_sem.at[slot]).start()

    spread = sorted(range(1, n), key=lambda k: (abs(k - half), k))
    ring = [lax.rem(me + k, n) for k in spread]
    def main_one(i, target):
        ref = (packs + pair)[i]
        buf, send_sem, recv_sem, at = (kv_buf, kv_send, kv_recv, i) if i < 4 else (q_buf, q_send, q_recv, i - 4)
        send(ref.at[:, cols(target)], buf.at[me, :, lane(at)], send_sem.at[target], recv_sem.at[me], target)

    def extra_one(i, k, e):
        if i < 4:
            extra_send(packs[i], i, xkv_buf, me, xkv_send.at[k, e], xkv_recv, side if k else 1 - side, e)
        elif k:
            extra_send(pair[i - 4], i - 4, xq_buf, place, xq_send.at[e], xq_recv, side, e)

    turns = [lax.rem(me + e, extra) for e in range(extra)]
    for token, i in ORDER:
        if token == "M":
            for target in ring:
                main_one(i, target)
        elif token == "Q":
            for target in ring:
                main_one(4, target)
                main_one(5, target)
        elif token == "X":
            for k in (0, 1):
                for e in turns:
                    extra_one(i, k, e)
        elif token == "C":
            for e in turns:
                extra_one(i, 0, e)
        elif token == "L":
            for e in turns:
                extra_one(i, 1, e)
        elif token == "B":
            for target in ring:
                send(bias_ref, bias_buf.at[me], b_send.at[target], b_recv.at[me], target)
            pltpu.make_async_copy(bias_ref, bias_buf.at[me], b_recv.at[me]).start()
            for i, ref in enumerate(packs):
                pltpu.make_async_copy(ref.at[:, cols(me)], kv_buf.at[me, :, lane(i)], kv_recv.at[me]).start()
            for i, ref in enumerate(pair):
                pltpu.make_async_copy(ref.at[:, cols(me)], q_buf.at[me, :, lane(i)], q_recv.at[me]).start()

    def each(low, high, step):
        def run(i, carried):
            step(i)
            return carried

        lax.fori_loop(low, high, run, 0)

    each(0, n, lambda i: wait(bias_buf.at[i], b_recv.at[i]))

    is_host = jnp.logical_and(me >= first_host, me < first_host + 2 * extra)
    mine = lax.rem(me - first_host + n * extra, extra)
    outs = (o_ref, ot_ref)

    def put(buf, slot, send_sem, recv_sem, source, head, target):
        @pl.when(target != me)
        def _():
            for i, ref in enumerate(outs):
                send(buf.at[slot, :, lane(i)], ref.at[:, cols(head)], send_sem.at[slot], recv_sem.at[source], target)

        @pl.when(target == me)
        def _():
            for i, ref in enumerate(outs):
                pltpu.make_async_copy(buf.at[slot, :, lane(i)], ref.at[:, cols(head)], recv_sem.at[source]).start()

    @pl.when(is_host)
    def _():
        each(0, n, lambda i: wait(xkv_buf.at[i], xkv_recv.at[i]))
        each(0, half, lambda i: wait(xq_buf.at[i], xq_recv.at[i]))

        def step(i):
            shard = side * half + i
            output, tangent = attend(shard, i, n, xq_buf, xkv_buf, bias_buf, s_buf)
            xout_buf[i, :, 0:d] = output
            xout_buf[i, :, d : 2 * d] = tangent
            put(xout_buf, i, xo_send, xo_recv, mine, n + mine, shard)

        each(0, half, step)

    each(0, n, lambda i: wait(kv_buf.at[i], kv_recv.at[i]))

    def order(i):
        ahead = (i + 1) // 2
        return lax.rem(me + half + n + ahead * (1 - 2 * lax.rem(i, 2)), n)

    def main_step(i):
        shard = order(i)
        wait(q_buf.at[shard], q_recv.at[shard])
        output, tangent = attend(shard, shard, n, q_buf, kv_buf, bias_buf, s_buf)
        out_buf[shard, :, 0:d] = output
        out_buf[shard, :, d : 2 * d] = tangent
        put(out_buf, shard, o_send, o_recv, me, me, shard)

    each(0, n, main_step)

    each(0, n, lambda i: wait(out_buf.at[i], o_recv.at[i]))
    each(0, extra, lambda i: wait(xout_buf.at[i], xo_recv.at[i]))

    def drain(i):
        target = lax.rem(me + i, n)
        wait(kv_buf.at[target], kv_send.at[target])
        wait(q_buf.at[target], q_send.at[target])
        wait(bias_buf.at[target], b_send.at[target])
        wait(out_buf.at[target], o_send.at[target])

    each(1, n, drain)
    for e in range(extra):
        @pl.when(host(1 - side, e) != me)
        def _():
            wait(xkv_buf.at[0], xkv_send.at[0, e])

        @pl.when(host(side, e) != me)
        def _():
            wait(xkv_buf.at[0], xkv_send.at[1, e])
            wait(xq_buf.at[0], xq_send.at[e])

    @pl.when(is_host)
    def _():
        def step(i):
            @pl.when(side * half + i != me)
            def _():
                wait(xout_buf.at[i], xo_send.at[i])

        each(0, half, step)


def store_kernel(a_ref, b_ref, o_ref, ot_ref, sems):
    moves = [
        pltpu.make_async_copy(a_ref, o_ref, sems.at[0]),
        pltpu.make_async_copy(b_ref, ot_ref, sems.at[1]),
    ]
    for move in moves:
        move.start()
    for move in moves:
        move.wait()


def exchanged(n, queries, query_tangents, keys, key_tangents, values, value_tangents, selection):
    rows, width = queries.shape
    half, extra, d = n // 2, HEADS - n, HEAD_DIM
    vm = pltpu.VMEM
    dma = pltpu.SemaphoreType.DMA
    reach = 2 * REACH + 1
    bf = jnp.bfloat16
    landed = pl.pallas_call(
        functools.partial(exchange_kernel, n),
        out_shape=[vm((rows, width), bf)] * 2,
        in_specs=[pl.BlockSpec(memory_space=pl.ANY)] * 7,
        out_specs=[pl.BlockSpec(memory_space=vm)] * 2,
        scratch_shapes=[
            vm((n, rows, 2 * d), bf),
            vm((n, rows, 4 * d), bf),
            vm((half, rows, 2 * d), bf),
            vm((n, rows, 4 * d), bf),
            vm((n,) + selection.shape, jnp.int32),
            vm((n, rows, 2 * d), bf),
            vm((half, rows, 2 * d), bf),
            vm((reach, rows, rows), jnp.float32),
            dma((n,)), dma((n,)), dma((n,)), dma((n,)), dma((2, extra)), dma((extra,)), dma((half,)),
            dma((n,)), dma((n,)), dma((n,)), dma((n,)), dma((n,)), dma((half,)), dma((extra,)),
        ],
        compiler_params=pltpu.CompilerParams(
            collective_id=0, has_side_effects=True, vmem_limit_bytes=67_043_328 - 4 * rows * width - 131_072
        ),
        name="exchange",
    )(queries, query_tangents, keys, key_tangents, values, value_tangents, selection)
    return pl.pallas_call(
        store_kernel,
        out_shape=[jax.ShapeDtypeStruct((rows, width), bf)] * 2,
        in_specs=[pl.BlockSpec(memory_space=vm)] * 2,
        out_specs=[pl.BlockSpec(memory_space=pl.ANY)] * 2,
        scratch_shapes=[dma((2,))],
        name="store",
    )(*[pltpu.with_memory_space_constraint(x, vm) for x in landed])


def solution(mesh):
    n = mesh.shape["ctx"]
    covered = n == 2 * REACH + 2 and n < HEADS and 2 * (HEADS - n) <= n
    placed = (
        P("ctx", "head"),
        P("ctx", "head"),
        P("ctx", "head"),
        P("ctx", "head"),
        P("ctx", "head"),
        P("ctx", "head"),
        P("ctx", None),
    )
    return jax.shard_map(
        functools.partial(exchanged, n) if covered else body,
        mesh=mesh,
        in_specs=placed,
        out_specs=(P("ctx", "head"), P("ctx", "head")),
        check_vma=False,
    )
```

```python
import functools

import jax
import jax.numpy as jnp
from jax import lax
from jax.sharding import PartitionSpec as P
from jax.experimental import pallas as pl
from jax.experimental.pallas import tpu as pltpu

HEADS = 10
HEAD_DIM = 128
BLK = 128
REACH = 3


big_negative = -1e30


def from_behind(array, axis, by):
    devices = lax.axis_size(axis)
    return lax.ppermute(array, axis, [(i, (i + by) % devices) for i in range(devices)])


def heads_view(flat_array):
    return flat_array.reshape(flat_array.shape[0], HEADS, HEAD_DIM)


def tile_update(accumulators, query_pieces, key_pieces):
    score_scale = HEAD_DIM ** (-0.5)
    query_block, query_tangent = query_pieces
    key_block, key_tangent, value_block, value_tangent = key_pieces
    running, weight_total, tangent_total, mixed_sum, mixed_tangent = accumulators
    scores = (
        jnp.einsum("qhd,khd->qhk", query_block, key_block, preferred_element_type=jnp.float32)
        * score_scale
    )
    score_tangents = (
        jnp.einsum("qhd,khd->qhk", query_tangent, key_block, preferred_element_type=jnp.float32)
        + jnp.einsum("qhd,khd->qhk", query_block, key_tangent, preferred_element_type=jnp.float32)
    ) * score_scale
    highest = jnp.maximum(running, scores.max(axis=2))
    factor = jnp.exp(running - highest)
    weights = jnp.exp(scores - highest[:, :, None])
    weighted = weights * score_tangents
    weight_total = factor * weight_total + weights.sum(axis=2)
    tangent_total = factor * tangent_total + weighted.sum(axis=2)
    rounded_weights = weights.astype(jnp.bfloat16)
    rounded_tangent = weighted.astype(jnp.bfloat16)
    mixed_sum = factor[:, :, None] * mixed_sum + jnp.einsum(
        "qhk,khd->qhd", rounded_weights, value_block, preferred_element_type=jnp.float32
    )
    mixed_tangent = (
        factor[:, :, None] * mixed_tangent
        + jnp.einsum(
            "qhk,khd->qhd", rounded_tangent, value_block, preferred_element_type=jnp.float32
        )
        + jnp.einsum(
            "qhk,khd->qhd", rounded_weights, value_tangent, preferred_element_type=jnp.float32
        )
    )
    return (highest, weight_total, tangent_total, mixed_sum, mixed_tangent)


def sweep(accumulators, query_pair, chosen_rows, key_pack, column_base):
    per_device = chosen_rows.shape[0]

    def visit(tile_index, carried):
        query_index = tile_index // per_device
        key_index = tile_index % per_device
        picked = chosen_rows[query_index, column_base + key_index] != 0

        def apply(carried_state):
            first_row = query_index * BLK
            pieces = tuple(
                (
                    lax.dynamic_slice_in_dim(full_array, first_row, BLK, 0)
                    for full_array in carried_state
                )
            )
            query_pieces = tuple(
                (
                    lax.dynamic_slice_in_dim(full_array, first_row, BLK, 0)
                    for full_array in query_pair
                )
            )
            key_pieces = tuple(
                (
                    lax.dynamic_slice_in_dim(full_array, key_index * BLK, BLK, 0)
                    for full_array in key_pack
                )
            )
            updated = tile_update(pieces, query_pieces, key_pieces)
            return tuple(
                (
                    lax.dynamic_update_slice_in_dim(full_array, new_piece, first_row, 0)
                    for full_array, new_piece in zip(carried_state, updated)
                )
            )

        return lax.cond(picked, apply, lambda unchanged: unchanged, carried)

    return lax.fori_loop(0, per_device * per_device, visit, tuple(accumulators))


def finish(accumulators):
    running, weight_total, tangent_total, mixed_sum, mixed_tangent = accumulators
    token_count = mixed_sum.shape[0]
    output = mixed_sum / weight_total[:, :, None]
    tangent = (mixed_tangent - output * tangent_total[:, :, None]) / weight_total[:, :, None]
    return (
        output.reshape(token_count, HEADS * HEAD_DIM).astype(jnp.bfloat16),
        tangent.reshape(token_count, HEADS * HEAD_DIM).astype(jnp.bfloat16),
    )


def body(queries, query_tangents, keys, key_tangents, values, value_tangents, selection):
    token_count = queries.shape[0]
    per_device = token_count // BLK
    query_pair = (heads_view(queries), heads_view(query_tangents))
    key_pack = (
        heads_view(keys),
        heads_view(key_tangents),
        heads_view(values),
        heads_view(value_tangents),
    )
    initial = (
        jnp.full((token_count, HEADS), big_negative, jnp.float32),
        jnp.zeros((token_count, HEADS), jnp.float32),
        jnp.zeros((token_count, HEADS), jnp.float32),
        jnp.zeros((token_count, HEADS, HEAD_DIM), jnp.float32),
        jnp.zeros((token_count, HEADS, HEAD_DIM), jnp.float32),
    )
    at_home = sweep(initial, query_pair, selection, key_pack, REACH * per_device)
    accumulators = at_home
    rising = key_pack
    falling = key_pack
    for offset in range(1, REACH + 1):
        rising = from_behind((rising[0], rising[1], rising[2], rising[3]), "ctx", -1)
        accumulators = sweep(
            accumulators, query_pair, selection, rising, (REACH + offset) * per_device
        )
        falling = from_behind((falling[0], falling[1], falling[2], falling[3]), "ctx", 1)
        accumulators = sweep(
            accumulators, query_pair, selection, falling, (REACH - offset) * per_device
        )
    return finish(accumulators)


ORDER = [('M', 0), ('B', 0), ('X', 0), ('M', 1), ('X', 1), ('M', 2), ('X', 2), ('M', 3), ('X', 3), ('X', 4), ('X', 5), ('M', 4), ('M', 5)]
HEAD_START = 3
LOG2E = 1.4426950408889634
MESH = pl.DeviceIdType.MESH


def attend(shard, q_slot, n, q_buf, kv_buf, bias_buf, s_buf):
    scale = HEAD_DIM ** (-0.5)
    factor = scale * LOG2E
    width = 2 * REACH + 1
    d = HEAD_DIM
    both = q_buf[q_slot]
    query = q_buf[q_slot, :, d : 2 * d]
    rows = both.shape[0]
    per_device = rows // BLK
    bias = jnp.where(bias_buf[shard] != 0, 0.0, big_negative)
    dims = (((1,), (1,)), ((), ()))
    slots = [lax.rem(shard + n - REACH + j, n) for j in range(width)]
    high = [None] * per_device
    for j in range(width):
        scores = lax.dot_general(
            query, kv_buf[slots[j], :, 0:d], dims, preferred_element_type=jnp.float32
        )
        for r in range(per_device):
            for k in range(per_device):
                column = j * per_device + k
                there = (slice(r * BLK, (r + 1) * BLK), slice(k * BLK, (k + 1) * BLK))
                masked = scores[there] * factor + bias[r : r + 1, column : column + 1]
                s_buf[(j,) + there] = masked
                high[r] = masked if high[r] is None else jnp.maximum(high[r], masked)
    peak = jnp.concatenate([jnp.max(h, axis=1, keepdims=True) for h in high], axis=0)
    total = jnp.zeros((rows, BLK), jnp.float32)
    tangent_total = jnp.zeros((rows, BLK), jnp.float32)
    mixed = jnp.zeros((rows, 2 * d), jnp.float32)
    mixed_tangent = jnp.zeros((rows, d), jnp.float32)
    for j in range(width):
        tangents = lax.dot_general(
            both, kv_buf[slots[j], :, 0 : 2 * d], dims, preferred_element_type=jnp.float32
        )
        weights = jnp.exp2(s_buf[j] - peak)
        weighted = weights * tangents
        for k in range(per_device):
            lanes = slice(k * BLK, (k + 1) * BLK)
            total = total + weights[:, lanes]
            tangent_total = tangent_total + weighted[:, lanes]
        mixed = mixed + jnp.dot(
            weights.astype(jnp.bfloat16),
            kv_buf[slots[j], :, 2 * d : 4 * d],
            preferred_element_type=jnp.float32,
        )
        mixed_tangent = mixed_tangent + jnp.dot(
            weighted.astype(jnp.bfloat16),
            kv_buf[slots[j], :, 2 * d : 3 * d],
            preferred_element_type=jnp.float32,
        )
    inverse = 1.0 / jnp.sum(total, axis=1, keepdims=True)
    tangent_sum = jnp.sum(tangent_total, axis=1, keepdims=True)
    output = mixed[:, 0:d] * inverse
    tangent = (scale * (mixed_tangent - output * tangent_sum) + mixed[:, d : 2 * d]) * inverse
    return output.astype(jnp.bfloat16), tangent.astype(jnp.bfloat16)


def exchange_kernel(
    n, q_ref, qt_ref, k_ref, kt_ref, v_ref, vt_ref, bias_ref, o_ref, ot_ref,
    q_buf, kv_buf, xq_buf, xkv_buf, bias_buf, out_buf, xout_buf, s_buf,
    kv_send, q_send, b_send, o_send, xkv_send, xq_send, xo_send,
    kv_recv, q_recv, b_recv, o_recv, xkv_recv, xq_recv, xo_recv, greet_sem,
):
    d = HEAD_DIM
    half = n // 2
    extra = HEADS - n
    me = lax.axis_index("ctx")
    side = me // half
    place = lax.rem(me, half)
    first_host = half - extra

    def cols(head):
        return pl.ds(pl.multiple_of(head * d, d), d)

    def host(which_side, e):
        return first_host + which_side * extra + e

    row, rows, y = me // 2, n // 2, lax.rem(me, 2)
    beside = 2 * row + 1 - y
    always = me >= 0

    def rows_away(by, column):
        return [(row + by < rows, 2 * (row + by) + column), (row >= by, 2 * (row - by) + column)]

    adjacent = [(always, beside)] + rows_away(1, y)
    second = rows_away(2, y) + rows_away(1, 1 - y)

    def greet(sem, group):
        count = jnp.int32(0)
        for there, target in group:
            count = count + there.astype(jnp.int32)

            @pl.when(there)
            def _():
                pl.semaphore_signal(sem, inc=1, device_id={"ctx": target}, device_id_type=MESH)

        pl.semaphore_wait(sem, count)

    greet(pltpu.get_barrier_semaphore(), adjacent)

    def send(src, dst, send_sem, recv_sem, target):
        pltpu.make_async_remote_copy(
            src_ref=src, dst_ref=dst, send_sem=send_sem, recv_sem=recv_sem,
            device_id={"ctx": target}, device_id_type=MESH,
        ).start()

    def wait(ref, sem):
        pltpu.make_async_copy(ref, ref, sem).wait()

    packs = (k_ref, kt_ref, v_ref, vt_ref)
    pair = (qt_ref, q_ref)

    def lane(i):
        return pl.ds(i * d, d)

    def extra_send(ref, i, buf, slot, send_sem, recv_sem, which_side, e):
        target = host(which_side, e)

        @pl.when(target != me)
        def _():
            send(ref.at[:, cols(n + e)], buf.at[slot, :, lane(i)], send_sem, recv_sem, target)

        @pl.when(target == me)
        def _():
            pltpu.make_async_copy(ref.at[:, cols(n + e)], buf.at[slot, :, lane(i)], recv_sem).start()

    spread = sorted(range(1, n), key=lambda k: (abs(k - half), k))
    ring = [lax.rem(me + k, n) for k in spread]
    def main_one(i, target):
        ref = (packs + pair)[i]
        buf, send_sem, recv_sem, at = (kv_buf, kv_send, kv_recv, i) if i < 4 else (q_buf, q_send, q_recv.at[me], i - 4)
        send(ref.at[:, cols(target)], buf.at[me, :, lane(at)], send_sem, recv_sem, target)

    def extra_one(i, k, e):
        if i < 4:
            extra_send(packs[i], i, xkv_buf, me, xkv_send.at[k, e], xkv_recv, side if k else 1 - side, e)
        elif k:
            extra_send(pair[i - 4], i - 4, xq_buf, place, xq_send.at[e], xq_recv, side, e)

    for i in range(HEAD_START):
        for there, target in adjacent:
            @pl.when(there)
            def _():
                main_one(i, target)

    greet(greet_sem.at[0], adjacent)
    greet(greet_sem.at[1], second)

    turns = [lax.rem(me + e, extra) for e in range(extra)]
    for token, i in ORDER:
        if token == "M":
            for target in ring:
                if i < HEAD_START:
                    near = functools.reduce(jnp.logical_or, [jnp.logical_and(there, t == target) for there, t in adjacent])

                    @pl.when(jnp.logical_not(near))
                    def _():
                        main_one(i, target)
                else:
                    main_one(i, target)
        elif token == "X":
            for k in (0, 1):
                for e in turns:
                    extra_one(i, k, e)
        elif token == "B":
            for target in ring:
                send(bias_ref, bias_buf.at[me], b_send, b_recv, target)
            pltpu.make_async_copy(bias_ref, bias_buf.at[me], b_recv).start()
            for i, ref in enumerate(packs):
                pltpu.make_async_copy(ref.at[:, cols(me)], kv_buf.at[me, :, lane(i)], kv_recv).start()
            for i, ref in enumerate(pair):
                pltpu.make_async_copy(ref.at[:, cols(me)], q_buf.at[me, :, lane(i)], q_recv.at[me]).start()

    def each(low, high, step):
        def run(i, carried):
            step(i)
            return carried

        lax.fori_loop(low, high, run, 0)

    wait(bias_buf, b_recv)

    is_host = jnp.logical_and(me >= first_host, me < first_host + 2 * extra)
    mine = lax.rem(me - first_host + n * extra, extra)
    outs = (o_ref, ot_ref)

    def put(buf, slot, send_sem, recv_sem, head, target):
        @pl.when(target != me)
        def _():
            for i, ref in enumerate(outs):
                send(buf.at[slot, :, lane(i)], ref.at[:, cols(head)], send_sem, recv_sem, target)

        @pl.when(target == me)
        def _():
            for i, ref in enumerate(outs):
                pltpu.make_async_copy(buf.at[slot, :, lane(i)], ref.at[:, cols(head)], recv_sem).start()

    @pl.when(is_host)
    def _():
        wait(xkv_buf, xkv_recv)
        wait(xq_buf, xq_recv)

        def step(i):
            shard = side * half + i
            output, tangent = attend(shard, i, n, xq_buf, xkv_buf, bias_buf, s_buf)
            xout_buf[i, :, 0:d] = output
            xout_buf[i, :, d : 2 * d] = tangent
            put(xout_buf, i, xo_send, xo_recv, n + mine, shard)

        each(0, half, step)

    wait(kv_buf, kv_recv)

    def order(i):
        ahead = (i + 1) // 2
        return lax.rem(me + half + n + ahead * (1 - 2 * lax.rem(i, 2)), n)

    def main_step(i):
        shard = order(i)
        wait(q_buf.at[shard], q_recv.at[shard])
        output, tangent = attend(shard, shard, n, q_buf, kv_buf, bias_buf, s_buf)
        out_buf[shard, :, 0:d] = output
        out_buf[shard, :, d : 2 * d] = tangent
        put(out_buf, shard, o_send, o_recv, me, shard)

    each(0, n, main_step)

    others = pl.ds(0, n - 1)
    wait(kv_buf.at[others], kv_send)
    wait(q_buf.at[others], q_send)
    wait(bias_buf.at[others], b_send)
    for e in range(extra):
        @pl.when(host(1 - side, e) != me)
        def _():
            wait(xkv_buf.at[0], xkv_send.at[0, e])

        @pl.when(host(side, e) != me)
        def _():
            wait(xkv_buf.at[0], xkv_send.at[1, e])
            wait(xq_buf.at[0], xq_send.at[e])

    @pl.when(is_host)
    def _():
        wait(xout_buf.at[pl.ds(0, half - 1)], xo_send)

    wait(xout_buf.at[pl.ds(0, extra)], xo_recv)
    wait(out_buf, o_recv)
    wait(out_buf.at[others], o_send)


def store_kernel(a_ref, b_ref, o_ref, ot_ref, sems):
    moves = [
        pltpu.make_async_copy(a_ref, o_ref, sems.at[0]),
        pltpu.make_async_copy(b_ref, ot_ref, sems.at[1]),
    ]
    for move in moves:
        move.start()
    for move in moves:
        move.wait()


def exchanged(n, queries, query_tangents, keys, key_tangents, values, value_tangents, selection):
    rows, width = queries.shape
    half, extra, d = n // 2, HEADS - n, HEAD_DIM
    vm = pltpu.VMEM
    dma = pltpu.SemaphoreType.DMA
    reach = 2 * REACH + 1
    bf = jnp.bfloat16
    landed = pl.pallas_call(
        functools.partial(exchange_kernel, n),
        out_shape=[vm((rows, width), bf)] * 2,
        in_specs=[pl.BlockSpec(memory_space=pl.ANY)] * 7,
        out_specs=[pl.BlockSpec(memory_space=vm)] * 2,
        scratch_shapes=[
            vm((n, rows, 2 * d), bf),
            vm((n, rows, 4 * d), bf),
            vm((half, rows, 2 * d), bf),
            vm((n, rows, 4 * d), bf),
            vm((n,) + selection.shape, jnp.int32),
            vm((n, rows, 2 * d), bf),
            vm((half, rows, 2 * d), bf),
            vm((reach, rows, rows), jnp.float32),
            dma, dma, dma, dma, dma((2, extra)), dma((extra,)), dma,
            dma, dma((n,)), dma, dma, dma, dma, dma,
            pltpu.SemaphoreType.REGULAR((2,)),
        ],
        compiler_params=pltpu.CompilerParams(
            collective_id=0, has_side_effects=True, vmem_limit_bytes=67_043_328 - 4 * rows * width - 131_072
        ),
        name="exchange",
    )(queries, query_tangents, keys, key_tangents, values, value_tangents, selection)
    return pl.pallas_call(
        store_kernel,
        out_shape=[jax.ShapeDtypeStruct((rows, width), bf)] * 2,
        in_specs=[pl.BlockSpec(memory_space=vm)] * 2,
        out_specs=[pl.BlockSpec(memory_space=pl.ANY)] * 2,
        scratch_shapes=[dma((2,))],
        name="store",
    )(*[pltpu.with_memory_space_constraint(x, vm) for x in landed])


def solution(mesh):
    n = mesh.shape["ctx"]
    covered = n == 2 * REACH + 2 and n < HEADS and 2 * (HEADS - n) <= n
    placed = (
        P("ctx", "head"),
        P("ctx", "head"),
        P("ctx", "head"),
        P("ctx", "head"),
        P("ctx", "head"),
        P("ctx", "head"),
        P("ctx", None),
    )
    return jax.shard_map(
        functools.partial(exchanged, n) if covered else body,
        mesh=mesh,
        in_specs=placed,
        out_specs=(P("ctx", "head"), P("ctx", "head")),
        check_vma=False,
    )
```

```python
import functools

import jax
import jax.numpy as jnp
from jax import lax
from jax.sharding import PartitionSpec as P
from jax.experimental import pallas as pl
from jax.experimental.pallas import tpu as pltpu

HEADS = 10
HEAD_DIM = 128
BLK = 128
REACH = 3


big_negative = -1e30


def from_behind(array, axis, by):
    devices = lax.axis_size(axis)
    return lax.ppermute(array, axis, [(i, (i + by) % devices) for i in range(devices)])


def heads_view(flat_array):
    return flat_array.reshape(flat_array.shape[0], HEADS, HEAD_DIM)


def tile_update(accumulators, query_pieces, key_pieces):
    score_scale = HEAD_DIM ** (-0.5)
    query_block, query_tangent = query_pieces
    key_block, key_tangent, value_block, value_tangent = key_pieces
    running, weight_total, tangent_total, mixed_sum, mixed_tangent = accumulators
    scores = (
        jnp.einsum("qhd,khd->qhk", query_block, key_block, preferred_element_type=jnp.float32)
        * score_scale
    )
    score_tangents = (
        jnp.einsum("qhd,khd->qhk", query_tangent, key_block, preferred_element_type=jnp.float32)
        + jnp.einsum("qhd,khd->qhk", query_block, key_tangent, preferred_element_type=jnp.float32)
    ) * score_scale
    highest = jnp.maximum(running, scores.max(axis=2))
    factor = jnp.exp(running - highest)
    weights = jnp.exp(scores - highest[:, :, None])
    weighted = weights * score_tangents
    weight_total = factor * weight_total + weights.sum(axis=2)
    tangent_total = factor * tangent_total + weighted.sum(axis=2)
    rounded_weights = weights.astype(jnp.bfloat16)
    rounded_tangent = weighted.astype(jnp.bfloat16)
    mixed_sum = factor[:, :, None] * mixed_sum + jnp.einsum(
        "qhk,khd->qhd", rounded_weights, value_block, preferred_element_type=jnp.float32
    )
    mixed_tangent = (
        factor[:, :, None] * mixed_tangent
        + jnp.einsum(
            "qhk,khd->qhd", rounded_tangent, value_block, preferred_element_type=jnp.float32
        )
        + jnp.einsum(
            "qhk,khd->qhd", rounded_weights, value_tangent, preferred_element_type=jnp.float32
        )
    )
    return (highest, weight_total, tangent_total, mixed_sum, mixed_tangent)


def sweep(accumulators, query_pair, chosen_rows, key_pack, column_base):
    per_device = chosen_rows.shape[0]

    def visit(tile_index, carried):
        query_index = tile_index // per_device
        key_index = tile_index % per_device
        picked = chosen_rows[query_index, column_base + key_index] != 0

        def apply(carried_state):
            first_row = query_index * BLK
            pieces = tuple(
                (
                    lax.dynamic_slice_in_dim(full_array, first_row, BLK, 0)
                    for full_array in carried_state
                )
            )
            query_pieces = tuple(
                (
                    lax.dynamic_slice_in_dim(full_array, first_row, BLK, 0)
                    for full_array in query_pair
                )
            )
            key_pieces = tuple(
                (
                    lax.dynamic_slice_in_dim(full_array, key_index * BLK, BLK, 0)
                    for full_array in key_pack
                )
            )
            updated = tile_update(pieces, query_pieces, key_pieces)
            return tuple(
                (
                    lax.dynamic_update_slice_in_dim(full_array, new_piece, first_row, 0)
                    for full_array, new_piece in zip(carried_state, updated)
                )
            )

        return lax.cond(picked, apply, lambda unchanged: unchanged, carried)

    return lax.fori_loop(0, per_device * per_device, visit, tuple(accumulators))


def finish(accumulators):
    running, weight_total, tangent_total, mixed_sum, mixed_tangent = accumulators
    token_count = mixed_sum.shape[0]
    output = mixed_sum / weight_total[:, :, None]
    tangent = (mixed_tangent - output * tangent_total[:, :, None]) / weight_total[:, :, None]
    return (
        output.reshape(token_count, HEADS * HEAD_DIM).astype(jnp.bfloat16),
        tangent.reshape(token_count, HEADS * HEAD_DIM).astype(jnp.bfloat16),
    )


def body(queries, query_tangents, keys, key_tangents, values, value_tangents, selection):
    token_count = queries.shape[0]
    per_device = token_count // BLK
    query_pair = (heads_view(queries), heads_view(query_tangents))
    key_pack = (
        heads_view(keys),
        heads_view(key_tangents),
        heads_view(values),
        heads_view(value_tangents),
    )
    initial = (
        jnp.full((token_count, HEADS), big_negative, jnp.float32),
        jnp.zeros((token_count, HEADS), jnp.float32),
        jnp.zeros((token_count, HEADS), jnp.float32),
        jnp.zeros((token_count, HEADS, HEAD_DIM), jnp.float32),
        jnp.zeros((token_count, HEADS, HEAD_DIM), jnp.float32),
    )
    at_home = sweep(initial, query_pair, selection, key_pack, REACH * per_device)
    accumulators = at_home
    rising = key_pack
    falling = key_pack
    for offset in range(1, REACH + 1):
        rising = from_behind((rising[0], rising[1], rising[2], rising[3]), "ctx", -1)
        accumulators = sweep(
            accumulators, query_pair, selection, rising, (REACH + offset) * per_device
        )
        falling = from_behind((falling[0], falling[1], falling[2], falling[3]), "ctx", 1)
        accumulators = sweep(
            accumulators, query_pair, selection, falling, (REACH - offset) * per_device
        )
    return finish(accumulators)


ORDER = [('M', 0), ('B', 0), ('X', 0), ('M', 1), ('X', 1), ('M', 2), ('X', 2), ('M', 3), ('X', 3), ('X', 4), ('X', 5), ('M', 4), ('M', 5)]
HEAD_START = 3
LOG2E = 1.4426950408889634
MESH = pl.DeviceIdType.MESH


def attend(shard, q_slot, n, q_buf, kv_buf, bias_buf, s_buf):
    scale = HEAD_DIM ** (-0.5)
    factor = scale * LOG2E
    width = 2 * REACH + 1
    d = HEAD_DIM
    both = q_buf[q_slot]
    query = q_buf[q_slot, :, d : 2 * d]
    rows = both.shape[0]
    per_device = rows // BLK
    bias = jnp.where(bias_buf[shard] != 0, 0.0, big_negative)
    dims = (((1,), (1,)), ((), ()))
    slots = [lax.rem(shard + n - REACH + j, n) for j in range(width)]
    high = [None] * per_device
    for j in range(width):
        scores = lax.dot_general(
            query, kv_buf[slots[j], :, 0:d], dims, preferred_element_type=jnp.float32
        )
        for r in range(per_device):
            for k in range(per_device):
                column = j * per_device + k
                there = (slice(r * BLK, (r + 1) * BLK), slice(k * BLK, (k + 1) * BLK))
                masked = scores[there] * factor + bias[r : r + 1, column : column + 1]
                s_buf[(j,) + there] = masked
                high[r] = masked if high[r] is None else jnp.maximum(high[r], masked)
    peak = jnp.concatenate([jnp.max(h, axis=1, keepdims=True) for h in high], axis=0)
    total = jnp.zeros((rows, BLK), jnp.float32)
    tangent_total = jnp.zeros((rows, BLK), jnp.float32)
    mixed = jnp.zeros((rows, 2 * d), jnp.float32)
    mixed_tangent = jnp.zeros((rows, d), jnp.float32)
    for j in range(width):
        tangents = lax.dot_general(
            both, kv_buf[slots[j], :, 0 : 2 * d], dims, preferred_element_type=jnp.float32
        )
        weights = jnp.exp2(s_buf[j] - peak)
        weighted = weights * tangents
        for k in range(per_device):
            lanes = slice(k * BLK, (k + 1) * BLK)
            total = total + weights[:, lanes]
            tangent_total = tangent_total + weighted[:, lanes]
        mixed = mixed + jnp.dot(
            weights.astype(jnp.bfloat16),
            kv_buf[slots[j], :, 2 * d : 4 * d],
            preferred_element_type=jnp.float32,
        )
        mixed_tangent = mixed_tangent + jnp.dot(
            weighted.astype(jnp.bfloat16),
            kv_buf[slots[j], :, 2 * d : 3 * d],
            preferred_element_type=jnp.float32,
        )
    inverse = 1.0 / jnp.sum(total, axis=1, keepdims=True)
    tangent_sum = jnp.sum(tangent_total, axis=1, keepdims=True)
    output = mixed[:, 0:d] * inverse
    tangent = (scale * (mixed_tangent - output * tangent_sum) + mixed[:, d : 2 * d]) * inverse
    return output.astype(jnp.bfloat16), tangent.astype(jnp.bfloat16)


def exchange_kernel(
    n, q_ref, qt_ref, k_ref, kt_ref, v_ref, vt_ref, bias_ref, o_ref, ot_ref,
    q_buf, kv_buf, xq_buf, xkv_buf, bias_buf, out_buf, xout_buf, s_buf,
    kv_send, q_send, b_send, o_send, xkv_send, xq_send, xo_send,
    kv_recv, q_recv, b_recv, o_recv, xkv_recv, xq_recv, xo_recv, greet_sem,
):
    d = HEAD_DIM
    half = n // 2
    extra = HEADS - n
    me = lax.axis_index("ctx")
    side = me // half
    place = lax.rem(me, half)
    first_host = half - extra

    def cols(head):
        return pl.ds(pl.multiple_of(head * d, d), d)

    def host(which_side, e):
        return first_host + which_side * extra + e

    row, rows, y = me // 2, n // 2, lax.rem(me, 2)
    is_inner = jnp.logical_and(row > 0, row < rows - 1)
    beside = 2 * row + 1 - y
    partner = 2 * (rows - 1 - row) + y
    along = 2 * jnp.where(row % 2 == 0, row + 1, row - 1) + y
    barrier = pltpu.get_barrier_semaphore()

    def signal(sem, target):
        pl.semaphore_signal(sem, inc=1, device_id={"ctx": target}, device_id_type=MESH)

    signal(barrier, jnp.where(is_inner, partner, beside))

    @pl.when(is_inner)
    def _():
        signal(barrier, along)

    pl.semaphore_wait(barrier, jnp.where(is_inner, 1, 2))

    def send(src, dst, send_sem, recv_sem, target):
        pltpu.make_async_remote_copy(
            src_ref=src, dst_ref=dst, send_sem=send_sem, recv_sem=recv_sem,
            device_id={"ctx": target}, device_id_type=MESH,
        ).start()

    def wait(ref, sem):
        pltpu.make_async_copy(ref, ref, sem).wait()

    packs = (k_ref, kt_ref, v_ref, vt_ref)
    pair = (qt_ref, q_ref)

    def lane(i):
        return pl.ds(i * d, d)

    def extra_send(ref, i, buf, slot, send_sem, recv_sem, which_side, e):
        target = host(which_side, e)

        @pl.when(target != me)
        def _():
            send(ref.at[:, cols(n + e)], buf.at[slot, :, lane(i)], send_sem, recv_sem, target)

        @pl.when(target == me)
        def _():
            pltpu.make_async_copy(ref.at[:, cols(n + e)], buf.at[slot, :, lane(i)], recv_sem).start()

    spread = sorted(range(1, n), key=lambda k: (abs(k - half), k))
    ring = [lax.rem(me + k, n) for k in spread]
    def main_one(i, target):
        ref = (packs + pair)[i]
        buf, send_sem, recv_sem, at = (kv_buf, kv_send, kv_recv, i) if i < 4 else (q_buf, q_send, q_recv.at[me], i - 4)
        send(ref.at[:, cols(target)], buf.at[me, :, lane(at)], send_sem, recv_sem, target)

    def extra_one(i, k, e):
        if i < 4:
            extra_send(packs[i], i, xkv_buf, me, xkv_send.at[k, e], xkv_recv, side if k else 1 - side, e)
        elif k:
            extra_send(pair[i - 4], i - 4, xq_buf, place, xq_send.at[e], xq_recv, side, e)

    def head_start(*targets):
        for i in range(HEAD_START):
            for target in targets:
                main_one(i, target)

    @pl.when(is_inner)
    def _():
        head_start(partner)
        pl.semaphore_wait(greet_sem.at[0], 1)
        signal(greet_sem.at[1], partner)
        head_start(along, beside)
        pl.semaphore_wait(greet_sem.at[1], 1)
        signal(greet_sem.at[1], along)

    @pl.when(jnp.logical_not(is_inner))
    def _():
        signal(greet_sem.at[0], beside)
        head_start(along, beside)
        pl.semaphore_wait(greet_sem.at[0], 1)
        signal(greet_sem.at[0], along)
        pl.semaphore_wait(greet_sem.at[1], 1)

    turns = [lax.rem(me + e, extra) for e in range(extra)]
    for token, i in ORDER:
        if token == "M":
            for target in ring:
                if i < HEAD_START:
                    near = functools.reduce(jnp.logical_or, [target == along, target == beside, jnp.logical_and(is_inner, target == partner)])

                    @pl.when(jnp.logical_not(near))
                    def _():
                        main_one(i, target)
                else:
                    main_one(i, target)
        elif token == "X":
            for k in (0, 1):
                for e in turns:
                    extra_one(i, k, e)
        elif token == "B":
            for target in ring:
                send(bias_ref, bias_buf.at[me], b_send, b_recv, target)
            pltpu.make_async_copy(bias_ref, bias_buf.at[me], b_recv).start()
            for i, ref in enumerate(packs):
                pltpu.make_async_copy(ref.at[:, cols(me)], kv_buf.at[me, :, lane(i)], kv_recv).start()
            for i, ref in enumerate(pair):
                pltpu.make_async_copy(ref.at[:, cols(me)], q_buf.at[me, :, lane(i)], q_recv.at[me]).start()

    def each(low, high, step):
        def run(i, carried):
            step(i)
            return carried

        lax.fori_loop(low, high, run, 0)

    wait(bias_buf, b_recv)

    is_host = jnp.logical_and(me >= first_host, me < first_host + 2 * extra)
    mine = lax.rem(me - first_host + n * extra, extra)
    outs = (o_ref, ot_ref)

    def put(buf, slot, send_sem, recv_sem, head, target):
        @pl.when(target != me)
        def _():
            for i, ref in enumerate(outs):
                send(buf.at[slot, :, lane(i)], ref.at[:, cols(head)], send_sem, recv_sem, target)

        @pl.when(target == me)
        def _():
            for i, ref in enumerate(outs):
                pltpu.make_async_copy(buf.at[slot, :, lane(i)], ref.at[:, cols(head)], recv_sem).start()

    @pl.when(is_host)
    def _():
        wait(xkv_buf, xkv_recv)
        wait(xq_buf, xq_recv)

        def step(i):
            shard = side * half + i
            output, tangent = attend(shard, i, n, xq_buf, xkv_buf, bias_buf, s_buf)
            xout_buf[i, :, 0:d] = output
            xout_buf[i, :, d : 2 * d] = tangent
            put(xout_buf, i, xo_send, xo_recv, n + mine, shard)

        each(0, half, step)

    wait(kv_buf, kv_recv)

    def order(i):
        ahead = (i + 1) // 2
        return lax.rem(me + half + n + ahead * (1 - 2 * lax.rem(i, 2)), n)

    def main_step(i):
        shard = order(i)
        wait(q_buf.at[shard], q_recv.at[shard])
        output, tangent = attend(shard, shard, n, q_buf, kv_buf, bias_buf, s_buf)
        out_buf[shard, :, 0:d] = output
        out_buf[shard, :, d : 2 * d] = tangent
        put(out_buf, shard, o_send, o_recv, me, shard)

    each(0, n, main_step)

    others = pl.ds(0, n - 1)
    wait(kv_buf.at[others], kv_send)
    wait(q_buf.at[others], q_send)
    wait(bias_buf.at[others], b_send)
    for e in range(extra):
        @pl.when(host(1 - side, e) != me)
        def _():
            wait(xkv_buf.at[0], xkv_send.at[0, e])

        @pl.when(host(side, e) != me)
        def _():
            wait(xkv_buf.at[0], xkv_send.at[1, e])
            wait(xq_buf.at[0], xq_send.at[e])

    @pl.when(is_host)
    def _():
        wait(xout_buf.at[pl.ds(0, half - 1)], xo_send)

    wait(xout_buf.at[pl.ds(0, extra)], xo_recv)
    wait(out_buf, o_recv)
    wait(out_buf.at[others], o_send)


def store_kernel(a_ref, b_ref, o_ref, ot_ref, sems):
    moves = [
        pltpu.make_async_copy(a_ref, o_ref, sems.at[0]),
        pltpu.make_async_copy(b_ref, ot_ref, sems.at[1]),
    ]
    for move in moves:
        move.start()
    for move in moves:
        move.wait()


def exchanged(n, queries, query_tangents, keys, key_tangents, values, value_tangents, selection):
    rows, width = queries.shape
    half, extra, d = n // 2, HEADS - n, HEAD_DIM
    vm = pltpu.VMEM
    dma = pltpu.SemaphoreType.DMA
    reach = 2 * REACH + 1
    bf = jnp.bfloat16
    landed = pl.pallas_call(
        functools.partial(exchange_kernel, n),
        out_shape=[vm((rows, width), bf)] * 2,
        in_specs=[pl.BlockSpec(memory_space=pl.ANY)] * 7,
        out_specs=[pl.BlockSpec(memory_space=vm)] * 2,
        scratch_shapes=[
            vm((n, rows, 2 * d), bf),
            vm((n, rows, 4 * d), bf),
            vm((half, rows, 2 * d), bf),
            vm((n, rows, 4 * d), bf),
            vm((n,) + selection.shape, jnp.int32),
            vm((n, rows, 2 * d), bf),
            vm((half, rows, 2 * d), bf),
            vm((reach, rows, rows), jnp.float32),
            dma, dma, dma, dma, dma((2, extra)), dma((extra,)), dma,
            dma, dma((n,)), dma, dma, dma, dma, dma,
            pltpu.SemaphoreType.REGULAR((2,)),
        ],
        compiler_params=pltpu.CompilerParams(
            collective_id=0, has_side_effects=True, vmem_limit_bytes=67_043_328 - 4 * rows * width - 131_072
        ),
        name="exchange",
    )(queries, query_tangents, keys, key_tangents, values, value_tangents, selection)
    return pl.pallas_call(
        store_kernel,
        out_shape=[jax.ShapeDtypeStruct((rows, width), bf)] * 2,
        in_specs=[pl.BlockSpec(memory_space=vm)] * 2,
        out_specs=[pl.BlockSpec(memory_space=pl.ANY)] * 2,
        scratch_shapes=[dma((2,))],
        name="store",
    )(*[pltpu.with_memory_space_constraint(x, vm) for x in landed])


def solution(mesh):
    n = mesh.shape["ctx"]
    covered = n == 2 * REACH + 2 and n < HEADS and 2 * (HEADS - n) <= n
    placed = (
        P("ctx", "head"),
        P("ctx", "head"),
        P("ctx", "head"),
        P("ctx", "head"),
        P("ctx", "head"),
        P("ctx", "head"),
        P("ctx", None),
    )
    return jax.shard_map(
        functools.partial(exchanged, n) if covered else body,
        mesh=mesh,
        in_specs=placed,
        out_specs=(P("ctx", "head"), P("ctx", "head")),
        check_vma=False,
    )
```

```python
import functools

import jax
import jax.numpy as jnp
from jax import lax
from jax.sharding import PartitionSpec as P
from jax.experimental import pallas as pl
from jax.experimental.pallas import tpu as pltpu

HEADS = 10
HEAD_DIM = 128
BLK = 128
REACH = 3


big_negative = -1e30


def from_behind(array, axis, by):
    devices = lax.axis_size(axis)
    return lax.ppermute(array, axis, [(i, (i + by) % devices) for i in range(devices)])


def heads_view(flat_array):
    return flat_array.reshape(flat_array.shape[0], HEADS, HEAD_DIM)


def tile_update(accumulators, query_pieces, key_pieces):
    score_scale = HEAD_DIM ** (-0.5)
    query_block, query_tangent = query_pieces
    key_block, key_tangent, value_block, value_tangent = key_pieces
    running, weight_total, tangent_total, mixed_sum, mixed_tangent = accumulators
    scores = (
        jnp.einsum("qhd,khd->qhk", query_block, key_block, preferred_element_type=jnp.float32)
        * score_scale
    )
    score_tangents = (
        jnp.einsum("qhd,khd->qhk", query_tangent, key_block, preferred_element_type=jnp.float32)
        + jnp.einsum("qhd,khd->qhk", query_block, key_tangent, preferred_element_type=jnp.float32)
    ) * score_scale
    highest = jnp.maximum(running, scores.max(axis=2))
    factor = jnp.exp(running - highest)
    weights = jnp.exp(scores - highest[:, :, None])
    weighted = weights * score_tangents
    weight_total = factor * weight_total + weights.sum(axis=2)
    tangent_total = factor * tangent_total + weighted.sum(axis=2)
    rounded_weights = weights.astype(jnp.bfloat16)
    rounded_tangent = weighted.astype(jnp.bfloat16)
    mixed_sum = factor[:, :, None] * mixed_sum + jnp.einsum(
        "qhk,khd->qhd", rounded_weights, value_block, preferred_element_type=jnp.float32
    )
    mixed_tangent = (
        factor[:, :, None] * mixed_tangent
        + jnp.einsum(
            "qhk,khd->qhd", rounded_tangent, value_block, preferred_element_type=jnp.float32
        )
        + jnp.einsum(
            "qhk,khd->qhd", rounded_weights, value_tangent, preferred_element_type=jnp.float32
        )
    )
    return (highest, weight_total, tangent_total, mixed_sum, mixed_tangent)


def sweep(accumulators, query_pair, chosen_rows, key_pack, column_base):
    per_device = chosen_rows.shape[0]

    def visit(tile_index, carried):
        query_index = tile_index // per_device
        key_index = tile_index % per_device
        picked = chosen_rows[query_index, column_base + key_index] != 0

        def apply(carried_state):
            first_row = query_index * BLK
            pieces = tuple(
                (
                    lax.dynamic_slice_in_dim(full_array, first_row, BLK, 0)
                    for full_array in carried_state
                )
            )
            query_pieces = tuple(
                (
                    lax.dynamic_slice_in_dim(full_array, first_row, BLK, 0)
                    for full_array in query_pair
                )
            )
            key_pieces = tuple(
                (
                    lax.dynamic_slice_in_dim(full_array, key_index * BLK, BLK, 0)
                    for full_array in key_pack
                )
            )
            updated = tile_update(pieces, query_pieces, key_pieces)
            return tuple(
                (
                    lax.dynamic_update_slice_in_dim(full_array, new_piece, first_row, 0)
                    for full_array, new_piece in zip(carried_state, updated)
                )
            )

        return lax.cond(picked, apply, lambda unchanged: unchanged, carried)

    return lax.fori_loop(0, per_device * per_device, visit, tuple(accumulators))


def finish(accumulators):
    running, weight_total, tangent_total, mixed_sum, mixed_tangent = accumulators
    token_count = mixed_sum.shape[0]
    output = mixed_sum / weight_total[:, :, None]
    tangent = (mixed_tangent - output * tangent_total[:, :, None]) / weight_total[:, :, None]
    return (
        output.reshape(token_count, HEADS * HEAD_DIM).astype(jnp.bfloat16),
        tangent.reshape(token_count, HEADS * HEAD_DIM).astype(jnp.bfloat16),
    )


def body(queries, query_tangents, keys, key_tangents, values, value_tangents, selection):
    token_count = queries.shape[0]
    per_device = token_count // BLK
    query_pair = (heads_view(queries), heads_view(query_tangents))
    key_pack = (
        heads_view(keys),
        heads_view(key_tangents),
        heads_view(values),
        heads_view(value_tangents),
    )
    initial = (
        jnp.full((token_count, HEADS), big_negative, jnp.float32),
        jnp.zeros((token_count, HEADS), jnp.float32),
        jnp.zeros((token_count, HEADS), jnp.float32),
        jnp.zeros((token_count, HEADS, HEAD_DIM), jnp.float32),
        jnp.zeros((token_count, HEADS, HEAD_DIM), jnp.float32),
    )
    at_home = sweep(initial, query_pair, selection, key_pack, REACH * per_device)
    accumulators = at_home
    rising = key_pack
    falling = key_pack
    for offset in range(1, REACH + 1):
        rising = from_behind((rising[0], rising[1], rising[2], rising[3]), "ctx", -1)
        accumulators = sweep(
            accumulators, query_pair, selection, rising, (REACH + offset) * per_device
        )
        falling = from_behind((falling[0], falling[1], falling[2], falling[3]), "ctx", 1)
        accumulators = sweep(
            accumulators, query_pair, selection, falling, (REACH - offset) * per_device
        )
    return finish(accumulators)


ORDER = [('M', 0), ('B', 0), ('X', 0), ('M', 1), ('X', 1), ('M', 2), ('X', 2), ('M', 3), ('X', 3), ('X', 4), ('X', 5), ('M', 4), ('M', 5)]
HEAD_START = 3
STEPS = [(2, 0), (2, 1), (1, 1), (1, 0), (3, 1), (3, 0), (0, 1)]
INNER = [5, 4, 6, 7, 0, 1, 2, 3]
OUTER = [3, 2, 6, 7, 4, 5, 0, 1]
LOG2E = 1.4426950408889634
MESH = pl.DeviceIdType.MESH


def attend(shard, q_slot, n, q_buf, kv_buf, bias_buf, s_buf):
    scale = HEAD_DIM ** (-0.5)
    factor = scale * LOG2E
    width = 2 * REACH + 1
    d = HEAD_DIM
    both = q_buf[q_slot]
    query = q_buf[q_slot, :, d : 2 * d]
    rows = both.shape[0]
    per_device = rows // BLK
    bias = jnp.where(bias_buf[shard] != 0, 0.0, big_negative)
    dims = (((1,), (1,)), ((), ()))
    slots = [lax.rem(shard + n - REACH + j, n) for j in range(width)]
    high = [None] * per_device
    for j in range(width):
        scores = lax.dot_general(
            query, kv_buf[slots[j], :, 0:d], dims, preferred_element_type=jnp.float32
        )
        for r in range(per_device):
            for k in range(per_device):
                column = j * per_device + k
                there = (slice(r * BLK, (r + 1) * BLK), slice(k * BLK, (k + 1) * BLK))
                masked = scores[there] * factor + bias[r : r + 1, column : column + 1]
                s_buf[(j,) + there] = masked
                high[r] = masked if high[r] is None else jnp.maximum(high[r], masked)
    peak = jnp.concatenate([jnp.max(h, axis=1, keepdims=True) for h in high], axis=0)
    total = jnp.zeros((rows, BLK), jnp.float32)
    tangent_total = jnp.zeros((rows, BLK), jnp.float32)
    mixed = jnp.zeros((rows, 2 * d), jnp.float32)
    mixed_tangent = jnp.zeros((rows, d), jnp.float32)
    for j in range(width):
        tangents = lax.dot_general(
            both, kv_buf[slots[j], :, 0 : 2 * d], dims, preferred_element_type=jnp.float32
        )
        weights = jnp.exp2(s_buf[j] - peak)
        weighted = weights * tangents
        for k in range(per_device):
            lanes = slice(k * BLK, (k + 1) * BLK)
            total = total + weights[:, lanes]
            tangent_total = tangent_total + weighted[:, lanes]
        mixed = mixed + jnp.dot(
            weights.astype(jnp.bfloat16),
            kv_buf[slots[j], :, 2 * d : 4 * d],
            preferred_element_type=jnp.float32,
        )
        mixed_tangent = mixed_tangent + jnp.dot(
            weighted.astype(jnp.bfloat16),
            kv_buf[slots[j], :, 2 * d : 3 * d],
            preferred_element_type=jnp.float32,
        )
    inverse = 1.0 / jnp.sum(total, axis=1, keepdims=True)
    tangent_sum = jnp.sum(tangent_total, axis=1, keepdims=True)
    output = mixed[:, 0:d] * inverse
    tangent = (scale * (mixed_tangent - output * tangent_sum) + mixed[:, d : 2 * d]) * inverse
    return output.astype(jnp.bfloat16), tangent.astype(jnp.bfloat16)


def exchange_kernel(
    n, q_ref, qt_ref, k_ref, kt_ref, v_ref, vt_ref, bias_ref, o_ref, ot_ref,
    q_buf, kv_buf, xq_buf, xkv_buf, bias_buf, out_buf, xout_buf, s_buf,
    kv_send, q_send, b_send, o_send, xkv_send, xq_send, xo_send,
    kv_recv, q_recv, b_recv, o_recv, xkv_recv, xq_recv, xo_recv, greet_sem,
):
    d = HEAD_DIM
    half = n // 2
    extra = HEADS - n
    me = lax.axis_index("ctx")
    side = me // half
    place = lax.rem(me, half)
    first_host = half - extra

    def cols(head):
        return pl.ds(pl.multiple_of(head * d, d), d)

    def host(which_side, e):
        return first_host + which_side * extra + e

    row, rows, y = me // 2, n // 2, lax.rem(me, 2)
    is_inner = jnp.logical_and(row > 0, row < rows - 1)
    beside = 2 * row + 1 - y
    partner = 2 * (rows - 1 - row) + y
    along = 2 * jnp.where(row % 2 == 0, row + 1, row - 1) + y
    barrier = pltpu.get_barrier_semaphore()

    def signal(sem, target):
        pl.semaphore_signal(sem, inc=1, device_id={"ctx": target}, device_id_type=MESH)

    signal(barrier, jnp.where(is_inner, partner, beside))

    @pl.when(is_inner)
    def _():
        signal(barrier, along)

    pl.semaphore_wait(barrier, jnp.where(is_inner, 1, 2))

    def send(src, dst, send_sem, recv_sem, target):
        pltpu.make_async_remote_copy(
            src_ref=src, dst_ref=dst, send_sem=send_sem, recv_sem=recv_sem,
            device_id={"ctx": target}, device_id_type=MESH,
        ).start()

    def wait(ref, sem):
        pltpu.make_async_copy(ref, ref, sem).wait()

    packs = (k_ref, kt_ref, v_ref, vt_ref)
    pair = (qt_ref, q_ref)

    def lane(i):
        return pl.ds(i * d, d)

    def extra_send(ref, i, buf, slot, send_sem, recv_sem, which_side, e):
        target = host(which_side, e)

        @pl.when(target != me)
        def _():
            send(ref.at[:, cols(n + e)], buf.at[slot, :, lane(i)], send_sem, recv_sem, target)

        @pl.when(target == me)
        def _():
            pltpu.make_async_copy(ref.at[:, cols(n + e)], buf.at[slot, :, lane(i)], recv_sem).start()

    toward = 1 - 2 * side
    ring = [
        2 * lax.rem(row + toward * dz + rows, rows) + (1 - y if dy else y) for dz, dy in STEPS
    ]

    def main_one(i, target):
        ref = (packs + pair)[i]
        buf, send_sem, recv_sem, at = (kv_buf, kv_send, kv_recv, i) if i < 4 else (q_buf, q_send, q_recv.at[me], i - 4)
        send(ref.at[:, cols(target)], buf.at[me, :, lane(at)], send_sem, recv_sem, target)

    def extra_one(i, k, e):
        if i < 4:
            extra_send(packs[i], i, xkv_buf, me, xkv_send.at[k, e], xkv_recv, side if k else 1 - side, e)
        elif k:
            extra_send(pair[i - 4], i - 4, xq_buf, place, xq_send.at[e], xq_recv, side, e)

    def head_start(*targets):
        for i in range(HEAD_START):
            for target in targets:
                main_one(i, target)

    @pl.when(is_inner)
    def _():
        head_start(partner)
        pl.semaphore_wait(greet_sem.at[0], 1)
        signal(greet_sem.at[1], partner)
        head_start(along, beside)
        pl.semaphore_wait(greet_sem.at[1], 1)
        signal(greet_sem.at[1], along)

    @pl.when(jnp.logical_not(is_inner))
    def _():
        signal(greet_sem.at[0], beside)
        head_start(along, beside)
        pl.semaphore_wait(greet_sem.at[0], 1)
        signal(greet_sem.at[0], along)
        pl.semaphore_wait(greet_sem.at[1], 1)

    turns = [lax.rem(me + e, extra) for e in range(extra)]
    for token, i in ORDER:
        if token == "M":
            for target in ring:
                if i < HEAD_START:
                    near = functools.reduce(jnp.logical_or, [target == along, target == beside, jnp.logical_and(is_inner, target == partner)])

                    @pl.when(jnp.logical_not(near))
                    def _():
                        main_one(i, target)
                else:
                    main_one(i, target)
        elif token == "X":
            for k in (0, 1):
                for e in turns:
                    extra_one(i, k, e)
        elif token == "B":
            for target in ring:
                send(bias_ref, bias_buf.at[me], b_send, b_recv, target)
            pltpu.make_async_copy(bias_ref, bias_buf.at[me], b_recv).start()
            for i, ref in enumerate(packs):
                pltpu.make_async_copy(ref.at[:, cols(me)], kv_buf.at[me, :, lane(i)], kv_recv).start()
            for i, ref in enumerate(pair):
                pltpu.make_async_copy(ref.at[:, cols(me)], q_buf.at[me, :, lane(i)], q_recv.at[me]).start()

    def each(low, high, step):
        def run(i, carried):
            step(i)
            return carried

        lax.fori_loop(low, high, run, 0)

    wait(bias_buf, b_recv)

    is_host = jnp.logical_and(me >= first_host, me < first_host + 2 * extra)
    mine = lax.rem(me - first_host + n * extra, extra)
    outs = (o_ref, ot_ref)

    def put(buf, slot, send_sem, recv_sem, head, target):
        @pl.when(target != me)
        def _():
            for i, ref in enumerate(outs):
                send(buf.at[slot, :, lane(i)], ref.at[:, cols(head)], send_sem, recv_sem, target)

        @pl.when(target == me)
        def _():
            for i, ref in enumerate(outs):
                pltpu.make_async_copy(buf.at[slot, :, lane(i)], ref.at[:, cols(head)], recv_sem).start()

    @pl.when(is_host)
    def _():
        wait(xkv_buf, xkv_recv)
        wait(xq_buf, xq_recv)

        def step(i):
            shard = side * half + i
            output, tangent = attend(shard, i, n, xq_buf, xkv_buf, bias_buf, s_buf)
            xout_buf[i, :, 0:d] = output
            xout_buf[i, :, d : 2 * d] = tangent
            put(xout_buf, i, xo_send, xo_recv, n + mine, shard)

        each(0, half, step)

    wait(kv_buf, kv_recv)

    def order(i):
        shard = me
        for k, (at_inner, at_outer) in enumerate(zip(INNER, OUTER)):
            target = jnp.where(is_inner, (*ring, me)[at_inner], (*ring, me)[at_outer])
            shard = jnp.where(i == k, target, shard)
        return shard

    def main_step(i):
        shard = order(i)
        wait(q_buf.at[shard], q_recv.at[shard])
        output, tangent = attend(shard, shard, n, q_buf, kv_buf, bias_buf, s_buf)
        out_buf[shard, :, 0:d] = output
        out_buf[shard, :, d : 2 * d] = tangent
        put(out_buf, shard, o_send, o_recv, me, shard)

    each(0, n, main_step)

    others = pl.ds(0, n - 1)
    wait(kv_buf.at[others], kv_send)
    wait(q_buf.at[others], q_send)
    wait(bias_buf.at[others], b_send)
    for e in range(extra):
        @pl.when(host(1 - side, e) != me)
        def _():
            wait(xkv_buf.at[0], xkv_send.at[0, e])

        @pl.when(host(side, e) != me)
        def _():
            wait(xkv_buf.at[0], xkv_send.at[1, e])
            wait(xq_buf.at[0], xq_send.at[e])

    @pl.when(is_host)
    def _():
        wait(xout_buf.at[pl.ds(0, half - 1)], xo_send)

    wait(xout_buf.at[pl.ds(0, extra)], xo_recv)
    wait(out_buf.at[others], o_send)
    wait(out_buf, o_recv)


def store_kernel(a_ref, b_ref, o_ref, ot_ref, sems):
    moves = [
        pltpu.make_async_copy(a_ref, o_ref, sems.at[0]),
        pltpu.make_async_copy(b_ref, ot_ref, sems.at[1]),
    ]
    for move in moves:
        move.start()
    for move in moves:
        move.wait()


def exchanged(n, queries, query_tangents, keys, key_tangents, values, value_tangents, selection):
    rows, width = queries.shape
    half, extra, d = n // 2, HEADS - n, HEAD_DIM
    vm = pltpu.VMEM
    dma = pltpu.SemaphoreType.DMA
    reach = 2 * REACH + 1
    bf = jnp.bfloat16
    landed = pl.pallas_call(
        functools.partial(exchange_kernel, n),
        out_shape=[vm((rows, width), bf)] * 2,
        in_specs=[pl.BlockSpec(memory_space=pl.ANY)] * 7,
        out_specs=[pl.BlockSpec(memory_space=vm)] * 2,
        scratch_shapes=[
            vm((n, rows, 2 * d), bf),
            vm((n, rows, 4 * d), bf),
            vm((half, rows, 2 * d), bf),
            vm((n, rows, 4 * d), bf),
            vm((n,) + selection.shape, jnp.int32),
            vm((n, rows, 2 * d), bf),
            vm((half, rows, 2 * d), bf),
            vm((reach, rows, rows), jnp.float32),
            dma, dma, dma, dma, dma((2, extra)), dma((extra,)), dma,
            dma, dma((n,)), dma, dma, dma, dma, dma,
            pltpu.SemaphoreType.REGULAR((2,)),
        ],
        compiler_params=pltpu.CompilerParams(
            collective_id=0, has_side_effects=True, vmem_limit_bytes=67_043_328 - 4 * rows * width - 131_072
        ),
        name="exchange",
    )(queries, query_tangents, keys, key_tangents, values, value_tangents, selection)
    return pl.pallas_call(
        store_kernel,
        out_shape=[jax.ShapeDtypeStruct((rows, width), bf)] * 2,
        in_specs=[pl.BlockSpec(memory_space=vm)] * 2,
        out_specs=[pl.BlockSpec(memory_space=pl.ANY)] * 2,
        scratch_shapes=[dma((2,))],
        name="store",
    )(*[pltpu.with_memory_space_constraint(x, vm) for x in landed])


def solution(mesh):
    n = mesh.shape["ctx"]
    covered = n == 2 * REACH + 2 and n < HEADS and 2 * (HEADS - n) <= n
    placed = (
        P("ctx", "head"),
        P("ctx", "head"),
        P("ctx", "head"),
        P("ctx", "head"),
        P("ctx", "head"),
        P("ctx", "head"),
        P("ctx", None),
    )
    return jax.shard_map(
        functools.partial(exchanged, n) if covered else body,
        mesh=mesh,
        in_specs=placed,
        out_specs=(P("ctx", "head"), P("ctx", "head")),
        check_vma=False,
    )
```

```python
import functools

import jax
import jax.numpy as jnp
from jax import lax
from jax.sharding import PartitionSpec as P
from jax.experimental import pallas as pl
from jax.experimental.pallas import tpu as pltpu

HEADS = 10
HEAD_DIM = 128
BLK = 128
REACH = 3


big_negative = -1e30


def from_behind(array, axis, by):
    devices = lax.axis_size(axis)
    return lax.ppermute(array, axis, [(i, (i + by) % devices) for i in range(devices)])


def heads_view(flat_array):
    return flat_array.reshape(flat_array.shape[0], HEADS, HEAD_DIM)


def tile_update(accumulators, query_pieces, key_pieces):
    score_scale = HEAD_DIM ** (-0.5)
    query_block, query_tangent = query_pieces
    key_block, key_tangent, value_block, value_tangent = key_pieces
    running, weight_total, tangent_total, mixed_sum, mixed_tangent = accumulators
    scores = (
        jnp.einsum("qhd,khd->qhk", query_block, key_block, preferred_element_type=jnp.float32)
        * score_scale
    )
    score_tangents = (
        jnp.einsum("qhd,khd->qhk", query_tangent, key_block, preferred_element_type=jnp.float32)
        + jnp.einsum("qhd,khd->qhk", query_block, key_tangent, preferred_element_type=jnp.float32)
    ) * score_scale
    highest = jnp.maximum(running, scores.max(axis=2))
    factor = jnp.exp(running - highest)
    weights = jnp.exp(scores - highest[:, :, None])
    weighted = weights * score_tangents
    weight_total = factor * weight_total + weights.sum(axis=2)
    tangent_total = factor * tangent_total + weighted.sum(axis=2)
    rounded_weights = weights.astype(jnp.bfloat16)
    rounded_tangent = weighted.astype(jnp.bfloat16)
    mixed_sum = factor[:, :, None] * mixed_sum + jnp.einsum(
        "qhk,khd->qhd", rounded_weights, value_block, preferred_element_type=jnp.float32
    )
    mixed_tangent = (
        factor[:, :, None] * mixed_tangent
        + jnp.einsum(
            "qhk,khd->qhd", rounded_tangent, value_block, preferred_element_type=jnp.float32
        )
        + jnp.einsum(
            "qhk,khd->qhd", rounded_weights, value_tangent, preferred_element_type=jnp.float32
        )
    )
    return (highest, weight_total, tangent_total, mixed_sum, mixed_tangent)


def sweep(accumulators, query_pair, chosen_rows, key_pack, column_base):
    per_device = chosen_rows.shape[0]

    def visit(tile_index, carried):
        query_index = tile_index // per_device
        key_index = tile_index % per_device
        picked = chosen_rows[query_index, column_base + key_index] != 0

        def apply(carried_state):
            first_row = query_index * BLK
            pieces = tuple(
                (
                    lax.dynamic_slice_in_dim(full_array, first_row, BLK, 0)
                    for full_array in carried_state
                )
            )
            query_pieces = tuple(
                (
                    lax.dynamic_slice_in_dim(full_array, first_row, BLK, 0)
                    for full_array in query_pair
                )
            )
            key_pieces = tuple(
                (
                    lax.dynamic_slice_in_dim(full_array, key_index * BLK, BLK, 0)
                    for full_array in key_pack
                )
            )
            updated = tile_update(pieces, query_pieces, key_pieces)
            return tuple(
                (
                    lax.dynamic_update_slice_in_dim(full_array, new_piece, first_row, 0)
                    for full_array, new_piece in zip(carried_state, updated)
                )
            )

        return lax.cond(picked, apply, lambda unchanged: unchanged, carried)

    return lax.fori_loop(0, per_device * per_device, visit, tuple(accumulators))


def finish(accumulators):
    running, weight_total, tangent_total, mixed_sum, mixed_tangent = accumulators
    token_count = mixed_sum.shape[0]
    output = mixed_sum / weight_total[:, :, None]
    tangent = (mixed_tangent - output * tangent_total[:, :, None]) / weight_total[:, :, None]
    return (
        output.reshape(token_count, HEADS * HEAD_DIM).astype(jnp.bfloat16),
        tangent.reshape(token_count, HEADS * HEAD_DIM).astype(jnp.bfloat16),
    )


def body(queries, query_tangents, keys, key_tangents, values, value_tangents, selection):
    token_count = queries.shape[0]
    per_device = token_count // BLK
    query_pair = (heads_view(queries), heads_view(query_tangents))
    key_pack = (
        heads_view(keys),
        heads_view(key_tangents),
        heads_view(values),
        heads_view(value_tangents),
    )
    initial = (
        jnp.full((token_count, HEADS), big_negative, jnp.float32),
        jnp.zeros((token_count, HEADS), jnp.float32),
        jnp.zeros((token_count, HEADS), jnp.float32),
        jnp.zeros((token_count, HEADS, HEAD_DIM), jnp.float32),
        jnp.zeros((token_count, HEADS, HEAD_DIM), jnp.float32),
    )
    at_home = sweep(initial, query_pair, selection, key_pack, REACH * per_device)
    accumulators = at_home
    rising = key_pack
    falling = key_pack
    for offset in range(1, REACH + 1):
        rising = from_behind((rising[0], rising[1], rising[2], rising[3]), "ctx", -1)
        accumulators = sweep(
            accumulators, query_pair, selection, rising, (REACH + offset) * per_device
        )
        falling = from_behind((falling[0], falling[1], falling[2], falling[3]), "ctx", 1)
        accumulators = sweep(
            accumulators, query_pair, selection, falling, (REACH - offset) * per_device
        )
    return finish(accumulators)


ORDER = [('M', 0), ('B', 0), ('X', 0), ('X', 1), ('X', 2), ('X', 3), ('X', 4), ('X', 5), ('M', 1), ('M', 2), ('M', 3), ('M', 4), ('M', 5)]
HEAD_START = 3
STEPS = [(2, 0), (2, 1), (1, 1), (1, 0), (3, 1), (3, 0), (0, 1)]
INNER = [5, 4, 6, 7, 0, 1, 2, 3]
OUTER = [3, 2, 6, 7, 4, 5, 0, 1]
LOG2E = 1.4426950408889634
MESH = pl.DeviceIdType.MESH


def attend(shard, q_slot, n, q_buf, kv_buf, bias_buf, s_buf):
    scale = HEAD_DIM ** (-0.5)
    factor = scale * LOG2E
    width = 2 * REACH + 1
    d = HEAD_DIM
    both = q_buf[q_slot]
    query = q_buf[q_slot, :, d : 2 * d]
    rows = both.shape[0]
    per_device = rows // BLK
    bias = jnp.where(bias_buf[shard] != 0, 0.0, big_negative)
    dims = (((1,), (1,)), ((), ()))
    slots = [lax.rem(shard + n - REACH + j, n) for j in range(width)]
    high = [None] * per_device
    for j in range(width):
        scores = lax.dot_general(
            query, kv_buf[slots[j], :, 0:d], dims, preferred_element_type=jnp.float32
        )
        for r in range(per_device):
            for k in range(per_device):
                column = j * per_device + k
                there = (slice(r * BLK, (r + 1) * BLK), slice(k * BLK, (k + 1) * BLK))
                masked = scores[there] * factor + bias[r : r + 1, column : column + 1]
                s_buf[(j,) + there] = masked
                high[r] = masked if high[r] is None else jnp.maximum(high[r], masked)
    peak = jnp.concatenate([jnp.max(h, axis=1, keepdims=True) for h in high], axis=0)
    total = jnp.zeros((rows, BLK), jnp.float32)
    tangent_total = jnp.zeros((rows, BLK), jnp.float32)
    mixed = jnp.zeros((rows, 2 * d), jnp.float32)
    mixed_tangent = jnp.zeros((rows, d), jnp.float32)
    for j in range(width):
        tangents = lax.dot_general(
            both, kv_buf[slots[j], :, 0 : 2 * d], dims, preferred_element_type=jnp.float32
        )
        weights = jnp.exp2(s_buf[j] - peak)
        weighted = weights * tangents
        for k in range(per_device):
            lanes = slice(k * BLK, (k + 1) * BLK)
            total = total + weights[:, lanes]
            tangent_total = tangent_total + weighted[:, lanes]
        mixed = mixed + jnp.dot(
            weights.astype(jnp.bfloat16),
            kv_buf[slots[j], :, 2 * d : 4 * d],
            preferred_element_type=jnp.float32,
        )
        mixed_tangent = mixed_tangent + jnp.dot(
            weighted.astype(jnp.bfloat16),
            kv_buf[slots[j], :, 2 * d : 3 * d],
            preferred_element_type=jnp.float32,
        )
    inverse = 1.0 / jnp.sum(total, axis=1, keepdims=True)
    tangent_sum = jnp.sum(tangent_total, axis=1, keepdims=True)
    output = mixed[:, 0:d] * inverse
    tangent = (scale * (mixed_tangent - output * tangent_sum) + mixed[:, d : 2 * d]) * inverse
    return output.astype(jnp.bfloat16), tangent.astype(jnp.bfloat16)


def exchange_kernel(
    n, q_ref, qt_ref, k_ref, kt_ref, v_ref, vt_ref, bias_ref, o_ref, ot_ref,
    q_buf, kv_buf, xq_buf, xkv_buf, bias_buf, out_buf, xout_buf, s_buf,
    kv_send, q_send, b_send, o_send, xkv_send, xq_send, xo_send,
    kv_recv, q_recv, b_recv, o_recv, xkv_recv, xq_recv, xo_recv, greet_sem,
):
    d = HEAD_DIM
    half = n // 2
    extra = HEADS - n
    me = lax.axis_index("ctx")
    side = me // half
    place = lax.rem(me, half)
    first_host = half - extra

    def cols(head):
        return pl.ds(pl.multiple_of(head * d, d), d)

    def host(which_side, e):
        return first_host + which_side * extra + e

    row, rows, y = me // 2, n // 2, lax.rem(me, 2)
    is_inner = jnp.logical_and(row > 0, row < rows - 1)
    beside = 2 * row + 1 - y
    partner = 2 * (rows - 1 - row) + y
    along = 2 * jnp.where(row % 2 == 0, row + 1, row - 1) + y
    barrier = pltpu.get_barrier_semaphore()

    def signal(sem, target):
        pl.semaphore_signal(sem, inc=1, device_id={"ctx": target}, device_id_type=MESH)

    signal(barrier, jnp.where(is_inner, partner, beside))

    @pl.when(is_inner)
    def _():
        signal(barrier, along)

    pl.semaphore_wait(barrier, jnp.where(is_inner, 1, 2))

    def send(src, dst, send_sem, recv_sem, target):
        pltpu.make_async_remote_copy(
            src_ref=src, dst_ref=dst, send_sem=send_sem, recv_sem=recv_sem,
            device_id={"ctx": target}, device_id_type=MESH,
        ).start()

    def wait(ref, sem):
        pltpu.make_async_copy(ref, ref, sem).wait()

    packs = (k_ref, kt_ref, v_ref, vt_ref)
    pair = (qt_ref, q_ref)

    def lane(i):
        return pl.ds(i * d, d)

    def extra_send(ref, i, buf, slot, send_sem, recv_sem, which_side, e):
        target = host(which_side, e)

        @pl.when(target != me)
        def _():
            send(ref.at[:, cols(n + e)], buf.at[slot, :, lane(i)], send_sem, recv_sem, target)

        @pl.when(target == me)
        def _():
            pltpu.make_async_copy(ref.at[:, cols(n + e)], buf.at[slot, :, lane(i)], recv_sem).start()

    toward = 1 - 2 * side
    ring = [
        2 * lax.rem(row + toward * dz + rows, rows) + (1 - y if dy else y) for dz, dy in STEPS
    ]

    def main_one(i, target):
        ref = (packs + pair)[i]
        buf, send_sem, recv_sem, at = (kv_buf, kv_send, kv_recv, i) if i < 4 else (q_buf, q_send, q_recv.at[me], i - 4)
        send(ref.at[:, cols(target)], buf.at[me, :, lane(at)], send_sem, recv_sem, target)

    def extra_one(i, k, e):
        if i < 4:
            extra_send(packs[i], i, xkv_buf, me, xkv_send.at[k, e], xkv_recv, side if k else 1 - side, e)
        elif k:
            extra_send(pair[i - 4], i - 4, xq_buf, place, xq_send.at[e], xq_recv, side, e)

    def head_start(*targets):
        for i in range(HEAD_START):
            for target in targets:
                main_one(i, target)

    @pl.when(is_inner)
    def _():
        head_start(partner)
        pl.semaphore_wait(greet_sem.at[0], 1)
        signal(greet_sem.at[1], partner)
        head_start(along, beside)
        pl.semaphore_wait(greet_sem.at[1], 1)
        signal(greet_sem.at[1], along)

    @pl.when(jnp.logical_not(is_inner))
    def _():
        signal(greet_sem.at[0], beside)
        head_start(along, beside)
        pl.semaphore_wait(greet_sem.at[0], 1)
        signal(greet_sem.at[0], along)
        pl.semaphore_wait(greet_sem.at[1], 1)

    turns = [lax.rem(me + e, extra) for e in range(extra)]
    for token, i in ORDER:
        if token == "M":
            for target in ring:
                if i < HEAD_START:
                    near = functools.reduce(jnp.logical_or, [target == along, target == beside, jnp.logical_and(is_inner, target == partner)])

                    @pl.when(jnp.logical_not(near))
                    def _():
                        main_one(i, target)
                else:
                    main_one(i, target)
        elif token == "X":
            for k in (0, 1):
                for e in turns:
                    extra_one(i, k, e)
        elif token == "B":
            for target in ring:
                send(bias_ref, bias_buf.at[me], b_send, b_recv, target)
            pltpu.make_async_copy(bias_ref, bias_buf.at[me], b_recv).start()
            for i, ref in enumerate(packs):
                pltpu.make_async_copy(ref.at[:, cols(me)], kv_buf.at[me, :, lane(i)], kv_recv).start()
            for i, ref in enumerate(pair):
                pltpu.make_async_copy(ref.at[:, cols(me)], q_buf.at[me, :, lane(i)], q_recv.at[me]).start()

    def each(low, high, step):
        def run(i, carried):
            step(i)
            return carried

        lax.fori_loop(low, high, run, 0)

    wait(bias_buf, b_recv)

    is_host = jnp.logical_and(me >= first_host, me < first_host + 2 * extra)
    mine = lax.rem(me - first_host + n * extra, extra)
    outs = (o_ref, ot_ref)

    def put(buf, slot, send_sem, recv_sem, head, target):
        @pl.when(target != me)
        def _():
            for i, ref in enumerate(outs):
                send(buf.at[slot, :, lane(i)], ref.at[:, cols(head)], send_sem, recv_sem, target)

        @pl.when(target == me)
        def _():
            for i, ref in enumerate(outs):
                pltpu.make_async_copy(buf.at[slot, :, lane(i)], ref.at[:, cols(head)], recv_sem).start()

    @pl.when(is_host)
    def _():
        wait(xkv_buf, xkv_recv)
        wait(xq_buf, xq_recv)

        def step(i):
            shard = side * half + i
            output, tangent = attend(shard, i, n, xq_buf, xkv_buf, bias_buf, s_buf)
            xout_buf[i, :, 0:d] = output
            xout_buf[i, :, d : 2 * d] = tangent
            put(xout_buf, i, xo_send, xo_recv, n + mine, shard)

        each(0, half, step)

    wait(kv_buf, kv_recv)

    def order(i):
        shard = me
        for k, (at_inner, at_outer) in enumerate(zip(INNER, OUTER)):
            target = jnp.where(is_inner, (*ring, me)[at_inner], (*ring, me)[at_outer])
            shard = jnp.where(i == k, target, shard)
        return shard

    def main_step(i):
        shard = order(i)
        wait(q_buf.at[shard], q_recv.at[shard])
        output, tangent = attend(shard, shard, n, q_buf, kv_buf, bias_buf, s_buf)
        out_buf[shard, :, 0:d] = output
        out_buf[shard, :, d : 2 * d] = tangent
        put(out_buf, shard, o_send, o_recv, me, shard)

    each(0, n, main_step)

    others = pl.ds(0, n - 1)
    wait(kv_buf.at[others], kv_send)
    wait(q_buf.at[others], q_send)
    wait(bias_buf.at[others], b_send)
    for e in range(extra):
        @pl.when(host(1 - side, e) != me)
        def _():
            wait(xkv_buf.at[0], xkv_send.at[0, e])

        @pl.when(host(side, e) != me)
        def _():
            wait(xkv_buf.at[0], xkv_send.at[1, e])
            wait(xq_buf.at[0], xq_send.at[e])

    @pl.when(is_host)
    def _():
        wait(xout_buf.at[pl.ds(0, half - 1)], xo_send)

    wait(xout_buf.at[pl.ds(0, extra)], xo_recv)
    wait(out_buf.at[others], o_send)
    wait(out_buf, o_recv)


def store_kernel(a_ref, b_ref, o_ref, ot_ref, sems):
    moves = [
        pltpu.make_async_copy(a_ref, o_ref, sems.at[0]),
        pltpu.make_async_copy(b_ref, ot_ref, sems.at[1]),
    ]
    for move in moves:
        move.start()
    for move in moves:
        move.wait()


def exchanged(n, queries, query_tangents, keys, key_tangents, values, value_tangents, selection):
    rows, width = queries.shape
    half, extra, d = n // 2, HEADS - n, HEAD_DIM
    vm = pltpu.VMEM
    dma = pltpu.SemaphoreType.DMA
    reach = 2 * REACH + 1
    bf = jnp.bfloat16
    landed = pl.pallas_call(
        functools.partial(exchange_kernel, n),
        out_shape=[vm((rows, width), bf)] * 2,
        in_specs=[pl.BlockSpec(memory_space=pl.ANY)] * 7,
        out_specs=[pl.BlockSpec(memory_space=vm)] * 2,
        scratch_shapes=[
            vm((n, rows, 2 * d), bf),
            vm((n, rows, 4 * d), bf),
            vm((half, rows, 2 * d), bf),
            vm((n, rows, 4 * d), bf),
            vm((n,) + selection.shape, jnp.int32),
            vm((n, rows, 2 * d), bf),
            vm((half, rows, 2 * d), bf),
            vm((reach, rows, rows), jnp.float32),
            dma, dma, dma, dma, dma((2, extra)), dma((extra,)), dma,
            dma, dma((n,)), dma, dma, dma, dma, dma,
            pltpu.SemaphoreType.REGULAR((2,)),
        ],
        compiler_params=pltpu.CompilerParams(
            collective_id=0, has_side_effects=True, vmem_limit_bytes=67_043_328 - 4 * rows * width - 131_072
        ),
        name="exchange",
    )(queries, query_tangents, keys, key_tangents, values, value_tangents, selection)
    return pl.pallas_call(
        store_kernel,
        out_shape=[jax.ShapeDtypeStruct((rows, width), bf)] * 2,
        in_specs=[pl.BlockSpec(memory_space=vm)] * 2,
        out_specs=[pl.BlockSpec(memory_space=pl.ANY)] * 2,
        scratch_shapes=[dma((2,))],
        name="store",
    )(*[pltpu.with_memory_space_constraint(x, vm) for x in landed])


def solution(mesh):
    n = mesh.shape["ctx"]
    covered = n == 2 * REACH + 2 and n < HEADS and 2 * (HEADS - n) <= n
    placed = (
        P("ctx", "head"),
        P("ctx", "head"),
        P("ctx", "head"),
        P("ctx", "head"),
        P("ctx", "head"),
        P("ctx", "head"),
        P("ctx", None),
    )
    return jax.shard_map(
        functools.partial(exchanged, n) if covered else body,
        mesh=mesh,
        in_specs=placed,
        out_specs=(P("ctx", "head"), P("ctx", "head")),
        check_vma=False,
    )
```

```python
import functools

import jax
import jax.numpy as jnp
from jax import lax
from jax.sharding import PartitionSpec as P
from jax.experimental import pallas as pl
from jax.experimental.pallas import tpu as pltpu

HEADS = 10
HEAD_DIM = 128
BLK = 128
REACH = 3


big_negative = -1e30


def from_behind(array, axis, by):
    devices = lax.axis_size(axis)
    return lax.ppermute(array, axis, [(i, (i + by) % devices) for i in range(devices)])


def heads_view(flat_array):
    return flat_array.reshape(flat_array.shape[0], HEADS, HEAD_DIM)


def tile_update(accumulators, query_pieces, key_pieces):
    score_scale = HEAD_DIM ** (-0.5)
    query_block, query_tangent = query_pieces
    key_block, key_tangent, value_block, value_tangent = key_pieces
    running, weight_total, tangent_total, mixed_sum, mixed_tangent = accumulators
    scores = (
        jnp.einsum("qhd,khd->qhk", query_block, key_block, preferred_element_type=jnp.float32)
        * score_scale
    )
    score_tangents = (
        jnp.einsum("qhd,khd->qhk", query_tangent, key_block, preferred_element_type=jnp.float32)
        + jnp.einsum("qhd,khd->qhk", query_block, key_tangent, preferred_element_type=jnp.float32)
    ) * score_scale
    highest = jnp.maximum(running, scores.max(axis=2))
    factor = jnp.exp(running - highest)
    weights = jnp.exp(scores - highest[:, :, None])
    weighted = weights * score_tangents
    weight_total = factor * weight_total + weights.sum(axis=2)
    tangent_total = factor * tangent_total + weighted.sum(axis=2)
    rounded_weights = weights.astype(jnp.bfloat16)
    rounded_tangent = weighted.astype(jnp.bfloat16)
    mixed_sum = factor[:, :, None] * mixed_sum + jnp.einsum(
        "qhk,khd->qhd", rounded_weights, value_block, preferred_element_type=jnp.float32
    )
    mixed_tangent = (
        factor[:, :, None] * mixed_tangent
        + jnp.einsum(
            "qhk,khd->qhd", rounded_tangent, value_block, preferred_element_type=jnp.float32
        )
        + jnp.einsum(
            "qhk,khd->qhd", rounded_weights, value_tangent, preferred_element_type=jnp.float32
        )
    )
    return (highest, weight_total, tangent_total, mixed_sum, mixed_tangent)


def sweep(accumulators, query_pair, chosen_rows, key_pack, column_base):
    per_device = chosen_rows.shape[0]

    def visit(tile_index, carried):
        query_index = tile_index // per_device
        key_index = tile_index % per_device
        picked = chosen_rows[query_index, column_base + key_index] != 0

        def apply(carried_state):
            first_row = query_index * BLK
            pieces = tuple(
                (
                    lax.dynamic_slice_in_dim(full_array, first_row, BLK, 0)
                    for full_array in carried_state
                )
            )
            query_pieces = tuple(
                (
                    lax.dynamic_slice_in_dim(full_array, first_row, BLK, 0)
                    for full_array in query_pair
                )
            )
            key_pieces = tuple(
                (
                    lax.dynamic_slice_in_dim(full_array, key_index * BLK, BLK, 0)
                    for full_array in key_pack
                )
            )
            updated = tile_update(pieces, query_pieces, key_pieces)
            return tuple(
                (
                    lax.dynamic_update_slice_in_dim(full_array, new_piece, first_row, 0)
                    for full_array, new_piece in zip(carried_state, updated)
                )
            )

        return lax.cond(picked, apply, lambda unchanged: unchanged, carried)

    return lax.fori_loop(0, per_device * per_device, visit, tuple(accumulators))


def finish(accumulators):
    running, weight_total, tangent_total, mixed_sum, mixed_tangent = accumulators
    token_count = mixed_sum.shape[0]
    output = mixed_sum / weight_total[:, :, None]
    tangent = (mixed_tangent - output * tangent_total[:, :, None]) / weight_total[:, :, None]
    return (
        output.reshape(token_count, HEADS * HEAD_DIM).astype(jnp.bfloat16),
        tangent.reshape(token_count, HEADS * HEAD_DIM).astype(jnp.bfloat16),
    )


def body(queries, query_tangents, keys, key_tangents, values, value_tangents, selection):
    token_count = queries.shape[0]
    per_device = token_count // BLK
    query_pair = (heads_view(queries), heads_view(query_tangents))
    key_pack = (
        heads_view(keys),
        heads_view(key_tangents),
        heads_view(values),
        heads_view(value_tangents),
    )
    initial = (
        jnp.full((token_count, HEADS), big_negative, jnp.float32),
        jnp.zeros((token_count, HEADS), jnp.float32),
        jnp.zeros((token_count, HEADS), jnp.float32),
        jnp.zeros((token_count, HEADS, HEAD_DIM), jnp.float32),
        jnp.zeros((token_count, HEADS, HEAD_DIM), jnp.float32),
    )
    at_home = sweep(initial, query_pair, selection, key_pack, REACH * per_device)
    accumulators = at_home
    rising = key_pack
    falling = key_pack
    for offset in range(1, REACH + 1):
        rising = from_behind((rising[0], rising[1], rising[2], rising[3]), "ctx", -1)
        accumulators = sweep(
            accumulators, query_pair, selection, rising, (REACH + offset) * per_device
        )
        falling = from_behind((falling[0], falling[1], falling[2], falling[3]), "ctx", 1)
        accumulators = sweep(
            accumulators, query_pair, selection, falling, (REACH - offset) * per_device
        )
    return finish(accumulators)


ORDER = [('M', 0), ('X', 0), ('X', 1), ('X', 2), ('X', 3), ('X', 4), ('X', 5), ('B', 0), ('M', 1), ('M', 2), ('M', 3), ('M', 4), ('M', 5)]
HEAD_START = 3
STEPS = [(2, 1), (2, 0), (1, 1), (1, 0), (3, 1), (3, 0), (0, 1)]
INNER = [5, 4, 6, 7, 0, 1, 2, 3]
OUTER = [3, 2, 6, 7, 4, 5, 0, 1]
LOG2E = 1.4426950408889634
MESH = pl.DeviceIdType.MESH


def attend(shard, q_slot, n, q_buf, kv_buf, bias_buf, s_buf):
    scale = HEAD_DIM ** (-0.5)
    factor = scale * LOG2E
    width = 2 * REACH + 1
    d = HEAD_DIM
    both = q_buf[q_slot]
    query = q_buf[q_slot, :, d : 2 * d]
    rows = both.shape[0]
    per_device = rows // BLK
    bias = jnp.where(bias_buf[shard] != 0, 0.0, big_negative)
    dims = (((1,), (1,)), ((), ()))
    slots = [lax.rem(shard + n - REACH + j, n) for j in range(width)]
    high = [None] * per_device
    for j in range(width):
        scores = lax.dot_general(
            query, kv_buf[slots[j], :, 0:d], dims, preferred_element_type=jnp.float32
        )
        for r in range(per_device):
            for k in range(per_device):
                column = j * per_device + k
                there = (slice(r * BLK, (r + 1) * BLK), slice(k * BLK, (k + 1) * BLK))
                masked = scores[there] * factor + bias[r : r + 1, column : column + 1]
                s_buf[(j,) + there] = masked
                high[r] = masked if high[r] is None else jnp.maximum(high[r], masked)
    peak = jnp.concatenate([jnp.max(h, axis=1, keepdims=True) for h in high], axis=0)
    total = jnp.zeros((rows, BLK), jnp.float32)
    tangent_total = jnp.zeros((rows, BLK), jnp.float32)
    mixed = jnp.zeros((rows, 2 * d), jnp.float32)
    mixed_tangent = jnp.zeros((rows, d), jnp.float32)
    for j in range(width):
        tangents = lax.dot_general(
            both, kv_buf[slots[j], :, 0 : 2 * d], dims, preferred_element_type=jnp.float32
        )
        weights = jnp.exp2(s_buf[j] - peak)
        weighted = weights * tangents
        for k in range(per_device):
            lanes = slice(k * BLK, (k + 1) * BLK)
            total = total + weights[:, lanes]
            tangent_total = tangent_total + weighted[:, lanes]
        mixed = mixed + jnp.dot(
            weights.astype(jnp.bfloat16),
            kv_buf[slots[j], :, 2 * d : 4 * d],
            preferred_element_type=jnp.float32,
        )
        mixed_tangent = mixed_tangent + jnp.dot(
            weighted.astype(jnp.bfloat16),
            kv_buf[slots[j], :, 2 * d : 3 * d],
            preferred_element_type=jnp.float32,
        )
    inverse = 1.0 / jnp.sum(total, axis=1, keepdims=True)
    tangent_sum = jnp.sum(tangent_total, axis=1, keepdims=True)
    output = mixed[:, 0:d] * inverse
    tangent = (scale * (mixed_tangent - output * tangent_sum) + mixed[:, d : 2 * d]) * inverse
    return output.astype(jnp.bfloat16), tangent.astype(jnp.bfloat16)


def exchange_kernel(
    n, q_ref, qt_ref, k_ref, kt_ref, v_ref, vt_ref, bias_ref, o_ref, ot_ref,
    q_buf, kv_buf, xq_buf, xkv_buf, bias_buf, out_buf, xout_buf, s_buf,
    kv_send, q_send, b_send, o_send, xkv_send, xq_send, xo_send,
    kv_recv, q_recv, b_recv, o_recv, xkv_recv, xq_recv, xo_recv, greet_sem,
):
    d = HEAD_DIM
    half = n // 2
    extra = HEADS - n
    me = lax.axis_index("ctx")
    side = me // half
    place = lax.rem(me, half)
    first_host = half - extra

    def cols(head):
        return pl.ds(pl.multiple_of(head * d, d), d)

    def host(which_side, e):
        return first_host + which_side * extra + e

    row, rows, y = me // 2, n // 2, lax.rem(me, 2)
    is_inner = jnp.logical_and(row > 0, row < rows - 1)
    beside = 2 * row + 1 - y
    partner = 2 * (rows - 1 - row) + y
    along = 2 * jnp.where(row % 2 == 0, row + 1, row - 1) + y
    barrier = pltpu.get_barrier_semaphore()

    def signal(sem, target):
        pl.semaphore_signal(sem, inc=1, device_id={"ctx": target}, device_id_type=MESH)

    signal(barrier, jnp.where(is_inner, partner, beside))

    @pl.when(is_inner)
    def _():
        signal(barrier, along)

    pl.semaphore_wait(barrier, jnp.where(is_inner, 1, 2))

    def send(src, dst, send_sem, recv_sem, target):
        pltpu.make_async_remote_copy(
            src_ref=src, dst_ref=dst, send_sem=send_sem, recv_sem=recv_sem,
            device_id={"ctx": target}, device_id_type=MESH,
        ).start()

    def wait(ref, sem):
        pltpu.make_async_copy(ref, ref, sem).wait()

    packs = (k_ref, kt_ref, v_ref, vt_ref)
    pair = (qt_ref, q_ref)

    def lane(i):
        return pl.ds(i * d, d)

    def extra_send(ref, i, buf, slot, send_sem, recv_sem, which_side, e):
        target = host(which_side, e)

        @pl.when(target != me)
        def _():
            send(ref.at[:, cols(n + e)], buf.at[slot, :, lane(i)], send_sem, recv_sem, target)

        @pl.when(target == me)
        def _():
            pltpu.make_async_copy(ref.at[:, cols(n + e)], buf.at[slot, :, lane(i)], recv_sem).start()

    toward = 1 - 2 * side
    ring = [
        2 * lax.rem(row + toward * dz + rows, rows) + (1 - y if dy else y) for dz, dy in STEPS
    ]

    def main_one(i, target):
        ref = (packs + pair)[i]
        buf, send_sem, recv_sem, at = (kv_buf, kv_send, kv_recv, i) if i < 4 else (q_buf, q_send, q_recv.at[me], i - 4)
        send(ref.at[:, cols(target)], buf.at[me, :, lane(at)], send_sem, recv_sem, target)

    def extra_one(i, k, e):
        if i < 4:
            extra_send(packs[i], i, xkv_buf, me, xkv_send, xkv_recv, side if k else 1 - side, e)
        elif k:
            extra_send(pair[i - 4], i - 4, xq_buf, place, xq_send, xq_recv, side, e)

    def head_start(*targets):
        for i in range(HEAD_START):
            for target in targets:
                main_one(i, target)

    @pl.when(is_inner)
    def _():
        head_start(partner)
        pl.semaphore_wait(greet_sem.at[0], 1)
        signal(greet_sem.at[1], partner)
        head_start(along, beside)
        pl.semaphore_wait(greet_sem.at[1], 1)
        signal(greet_sem.at[1], along)

    @pl.when(jnp.logical_not(is_inner))
    def _():
        signal(greet_sem.at[0], beside)
        head_start(along, beside)
        pl.semaphore_wait(greet_sem.at[0], 1)
        signal(greet_sem.at[0], along)
        pl.semaphore_wait(greet_sem.at[1], 1)

    turns = [lax.rem(me + e, extra) for e in range(extra)]
    for token, i in ORDER:
        if token == "M":
            for target in ring:
                if i < HEAD_START:
                    near = functools.reduce(jnp.logical_or, [target == along, target == beside, jnp.logical_and(is_inner, target == partner)])

                    @pl.when(jnp.logical_not(near))
                    def _():
                        main_one(i, target)
                else:
                    main_one(i, target)
        elif token == "X":
            for k in (0, 1):
                for e in turns:
                    extra_one(i, k, e)
        elif token == "B":
            for target in ring:
                send(bias_ref, bias_buf.at[me], b_send, b_recv, target)
            pltpu.make_async_copy(bias_ref, bias_buf.at[me], b_recv).start()
            for i, ref in enumerate(packs):
                pltpu.make_async_copy(ref.at[:, cols(me)], kv_buf.at[me, :, lane(i)], kv_recv).start()
            for i, ref in enumerate(pair):
                pltpu.make_async_copy(ref.at[:, cols(me)], q_buf.at[me, :, lane(i)], q_recv.at[me]).start()

    def each(low, high, step):
        def run(i, carried):
            step(i)
            return carried

        lax.fori_loop(low, high, run, 0)

    wait(bias_buf, b_recv)

    is_host = jnp.logical_and(me >= first_host, me < first_host + 2 * extra)
    mine = lax.rem(me - first_host + n * extra, extra)
    outs = (o_ref, ot_ref)

    def put(buf, slot, send_sem, recv_sem, head, target):
        @pl.when(target != me)
        def _():
            for i, ref in enumerate(outs):
                send(buf.at[slot, :, lane(i)], ref.at[:, cols(head)], send_sem, recv_sem, target)

        @pl.when(target == me)
        def _():
            for i, ref in enumerate(outs):
                pltpu.make_async_copy(buf.at[slot, :, lane(i)], ref.at[:, cols(head)], recv_sem).start()

    @pl.when(is_host)
    def _():
        wait(xkv_buf, xkv_recv)
        wait(xq_buf, xq_recv)

        def step(i):
            shard = side * half + i
            output, tangent = attend(shard, i, n, xq_buf, xkv_buf, bias_buf, s_buf)
            xout_buf[i, :, 0:d] = output
            xout_buf[i, :, d : 2 * d] = tangent
            put(xout_buf, i, xo_send, xo_recv, n + mine, shard)

        each(0, half, step)

    wait(kv_buf, kv_recv)

    def order(i):
        shard = me
        for k, (at_inner, at_outer) in enumerate(zip(INNER, OUTER)):
            target = jnp.where(is_inner, (*ring, me)[at_inner], (*ring, me)[at_outer])
            shard = jnp.where(i == k, target, shard)
        return shard

    def main_step(i):
        shard = order(i)
        wait(q_buf.at[shard], q_recv.at[shard])
        output, tangent = attend(shard, shard, n, q_buf, kv_buf, bias_buf, s_buf)
        out_buf[shard, :, 0:d] = output
        out_buf[shard, :, d : 2 * d] = tangent
        put(out_buf, shard, o_send, o_recv, me, shard)

    each(0, n, main_step)

    others = pl.ds(0, n - 1)
    wait(kv_buf.at[others], kv_send)
    wait(q_buf.at[others], q_send)
    wait(bias_buf.at[others], b_send)
    @pl.when(is_host)
    def _():
        wait(xkv_buf.at[pl.ds(0, 2 * extra - 1)], xkv_send)
        wait(xq_buf.at[pl.ds(0, extra - 1)], xq_send)

    @pl.when(jnp.logical_not(is_host))
    def _():
        wait(xkv_buf.at[pl.ds(0, 2 * extra)], xkv_send)
        wait(xq_buf.at[pl.ds(0, extra)], xq_send)

    @pl.when(is_host)
    def _():
        wait(xout_buf.at[pl.ds(0, half - 1)], xo_send)

    wait(xout_buf.at[pl.ds(0, extra)], xo_recv)
    wait(out_buf.at[others], o_send)
    wait(out_buf, o_recv)


def store_kernel(a_ref, b_ref, o_ref, ot_ref, sems):
    moves = [
        pltpu.make_async_copy(a_ref, o_ref, sems.at[0]),
        pltpu.make_async_copy(b_ref, ot_ref, sems.at[1]),
    ]
    for move in moves:
        move.start()
    for move in moves:
        move.wait()


def exchanged(n, queries, query_tangents, keys, key_tangents, values, value_tangents, selection):
    rows, width = queries.shape
    half, extra, d = n // 2, HEADS - n, HEAD_DIM
    vm = pltpu.VMEM
    dma = pltpu.SemaphoreType.DMA
    reach = 2 * REACH + 1
    bf = jnp.bfloat16
    landed = pl.pallas_call(
        functools.partial(exchange_kernel, n),
        out_shape=[vm((rows, width), bf)] * 2,
        in_specs=[pl.BlockSpec(memory_space=pl.ANY)] * 7,
        out_specs=[pl.BlockSpec(memory_space=vm)] * 2,
        scratch_shapes=[
            vm((n, rows, 2 * d), bf),
            vm((n, rows, 4 * d), bf),
            vm((half, rows, 2 * d), bf),
            vm((n, rows, 4 * d), bf),
            vm((n,) + selection.shape, jnp.int32),
            vm((n, rows, 2 * d), bf),
            vm((half, rows, 2 * d), bf),
            vm((reach, rows, rows), jnp.float32),
            dma, dma, dma, dma, dma, dma, dma,
            dma, dma((n,)), dma, dma, dma, dma, dma,
            pltpu.SemaphoreType.REGULAR((2,)),
        ],
        compiler_params=pltpu.CompilerParams(
            collective_id=0, has_side_effects=True, vmem_limit_bytes=67_043_328 - 4 * rows * width - 131_072
        ),
        name="exchange",
    )(queries, query_tangents, keys, key_tangents, values, value_tangents, selection)
    return pl.pallas_call(
        store_kernel,
        out_shape=[jax.ShapeDtypeStruct((rows, width), bf)] * 2,
        in_specs=[pl.BlockSpec(memory_space=vm)] * 2,
        out_specs=[pl.BlockSpec(memory_space=pl.ANY)] * 2,
        scratch_shapes=[dma((2,))],
        name="store",
    )(*[pltpu.with_memory_space_constraint(x, vm) for x in landed])


def solution(mesh):
    n = mesh.shape["ctx"]
    covered = n == 2 * REACH + 2 and n < HEADS and 2 * (HEADS - n) <= n
    placed = (
        P("ctx", "head"),
        P("ctx", "head"),
        P("ctx", "head"),
        P("ctx", "head"),
        P("ctx", "head"),
        P("ctx", "head"),
        P("ctx", None),
    )
    return jax.shard_map(
        functools.partial(exchanged, n) if covered else body,
        mesh=mesh,
        in_specs=placed,
        out_specs=(P("ctx", "head"), P("ctx", "head")),
        check_vma=False,
    )
```

```python
import functools

import jax
import jax.numpy as jnp
from jax import lax
from jax.sharding import PartitionSpec as P
from jax.experimental import pallas as pl
from jax.experimental.pallas import tpu as pltpu

HEADS = 10
HEAD_DIM = 128
BLK = 128
REACH = 3


big_negative = -1e30


def from_behind(array, axis, by):
    devices = lax.axis_size(axis)
    return lax.ppermute(array, axis, [(i, (i + by) % devices) for i in range(devices)])


def heads_view(flat_array):
    return flat_array.reshape(flat_array.shape[0], HEADS, HEAD_DIM)


def tile_update(accumulators, query_pieces, key_pieces):
    score_scale = HEAD_DIM ** (-0.5)
    query_block, query_tangent = query_pieces
    key_block, key_tangent, value_block, value_tangent = key_pieces
    running, weight_total, tangent_total, mixed_sum, mixed_tangent = accumulators
    scores = (
        jnp.einsum("qhd,khd->qhk", query_block, key_block, preferred_element_type=jnp.float32)
        * score_scale
    )
    score_tangents = (
        jnp.einsum("qhd,khd->qhk", query_tangent, key_block, preferred_element_type=jnp.float32)
        + jnp.einsum("qhd,khd->qhk", query_block, key_tangent, preferred_element_type=jnp.float32)
    ) * score_scale
    highest = jnp.maximum(running, scores.max(axis=2))
    factor = jnp.exp(running - highest)
    weights = jnp.exp(scores - highest[:, :, None])
    weighted = weights * score_tangents
    weight_total = factor * weight_total + weights.sum(axis=2)
    tangent_total = factor * tangent_total + weighted.sum(axis=2)
    rounded_weights = weights.astype(jnp.bfloat16)
    rounded_tangent = weighted.astype(jnp.bfloat16)
    mixed_sum = factor[:, :, None] * mixed_sum + jnp.einsum(
        "qhk,khd->qhd", rounded_weights, value_block, preferred_element_type=jnp.float32
    )
    mixed_tangent = (
        factor[:, :, None] * mixed_tangent
        + jnp.einsum(
            "qhk,khd->qhd", rounded_tangent, value_block, preferred_element_type=jnp.float32
        )
        + jnp.einsum(
            "qhk,khd->qhd", rounded_weights, value_tangent, preferred_element_type=jnp.float32
        )
    )
    return (highest, weight_total, tangent_total, mixed_sum, mixed_tangent)


def sweep(accumulators, query_pair, chosen_rows, key_pack, column_base):
    per_device = chosen_rows.shape[0]

    def visit(tile_index, carried):
        query_index = tile_index // per_device
        key_index = tile_index % per_device
        picked = chosen_rows[query_index, column_base + key_index] != 0

        def apply(carried_state):
            first_row = query_index * BLK
            pieces = tuple(
                (
                    lax.dynamic_slice_in_dim(full_array, first_row, BLK, 0)
                    for full_array in carried_state
                )
            )
            query_pieces = tuple(
                (
                    lax.dynamic_slice_in_dim(full_array, first_row, BLK, 0)
                    for full_array in query_pair
                )
            )
            key_pieces = tuple(
                (
                    lax.dynamic_slice_in_dim(full_array, key_index * BLK, BLK, 0)
                    for full_array in key_pack
                )
            )
            updated = tile_update(pieces, query_pieces, key_pieces)
            return tuple(
                (
                    lax.dynamic_update_slice_in_dim(full_array, new_piece, first_row, 0)
                    for full_array, new_piece in zip(carried_state, updated)
                )
            )

        return lax.cond(picked, apply, lambda unchanged: unchanged, carried)

    return lax.fori_loop(0, per_device * per_device, visit, tuple(accumulators))


def finish(accumulators):
    running, weight_total, tangent_total, mixed_sum, mixed_tangent = accumulators
    token_count = mixed_sum.shape[0]
    output = mixed_sum / weight_total[:, :, None]
    tangent = (mixed_tangent - output * tangent_total[:, :, None]) / weight_total[:, :, None]
    return (
        output.reshape(token_count, HEADS * HEAD_DIM).astype(jnp.bfloat16),
        tangent.reshape(token_count, HEADS * HEAD_DIM).astype(jnp.bfloat16),
    )


def body(queries, query_tangents, keys, key_tangents, values, value_tangents, selection):
    token_count = queries.shape[0]
    per_device = token_count // BLK
    query_pair = (heads_view(queries), heads_view(query_tangents))
    key_pack = (
        heads_view(keys),
        heads_view(key_tangents),
        heads_view(values),
        heads_view(value_tangents),
    )
    initial = (
        jnp.full((token_count, HEADS), big_negative, jnp.float32),
        jnp.zeros((token_count, HEADS), jnp.float32),
        jnp.zeros((token_count, HEADS), jnp.float32),
        jnp.zeros((token_count, HEADS, HEAD_DIM), jnp.float32),
        jnp.zeros((token_count, HEADS, HEAD_DIM), jnp.float32),
    )
    at_home = sweep(initial, query_pair, selection, key_pack, REACH * per_device)
    accumulators = at_home
    rising = key_pack
    falling = key_pack
    for offset in range(1, REACH + 1):
        rising = from_behind((rising[0], rising[1], rising[2], rising[3]), "ctx", -1)
        accumulators = sweep(
            accumulators, query_pair, selection, rising, (REACH + offset) * per_device
        )
        falling = from_behind((falling[0], falling[1], falling[2], falling[3]), "ctx", 1)
        accumulators = sweep(
            accumulators, query_pair, selection, falling, (REACH - offset) * per_device
        )
    return finish(accumulators)


ORDER = [('M', 0), ('B', 0), ('X', 0), ('X', 1), ('X', 2), ('X', 3), ('X', 4), ('X', 5), ('M', 1), ('M', 2), ('M', 3), ('M', 4), ('M', 5)]
HEAD_START = 3
STEPS = [(2, 0), (2, 1), (1, 1), (1, 0), (3, 1), (3, 0), (0, 1)]
INNER = [5, 4, 6, 7, 0, 1, 2, 3]
OUTER = [3, 2, 6, 7, 0, 1, 4, 5]
LOG2E = 1.4426950408889634
MESH = pl.DeviceIdType.MESH


def attend(shard, q_slot, n, q_buf, kv_buf, bias_buf, s_buf):
    scale = HEAD_DIM ** (-0.5)
    factor = scale * LOG2E
    width = 2 * REACH + 1
    d = HEAD_DIM
    both = q_buf[q_slot]
    query = q_buf[q_slot, :, d : 2 * d]
    rows = both.shape[0]
    per_device = rows // BLK
    bias = jnp.where(bias_buf[shard] != 0, 0.0, big_negative)
    dims = (((1,), (1,)), ((), ()))
    slots = [lax.rem(shard + n - REACH + j, n) for j in range(width)]
    high = [None] * per_device
    for j in range(width):
        scores = lax.dot_general(
            query, kv_buf[slots[j], :, 0:d], dims, preferred_element_type=jnp.float32
        )
        for r in range(per_device):
            for k in range(per_device):
                column = j * per_device + k
                there = (slice(r * BLK, (r + 1) * BLK), slice(k * BLK, (k + 1) * BLK))
                masked = scores[there] * factor + bias[r : r + 1, column : column + 1]
                s_buf[(j,) + there] = masked
                high[r] = masked if high[r] is None else jnp.maximum(high[r], masked)
    peak = jnp.concatenate([jnp.max(h, axis=1, keepdims=True) for h in high], axis=0)
    total = jnp.zeros((rows, BLK), jnp.float32)
    tangent_total = jnp.zeros((rows, BLK), jnp.float32)
    mixed = jnp.zeros((rows, 2 * d), jnp.float32)
    mixed_tangent = jnp.zeros((rows, d), jnp.float32)
    for j in range(width):
        tangents = lax.dot_general(
            both, kv_buf[slots[j], :, 0 : 2 * d], dims, preferred_element_type=jnp.float32
        )
        weights = jnp.exp2(s_buf[j] - peak)
        weighted = weights * tangents
        for k in range(per_device):
            lanes = slice(k * BLK, (k + 1) * BLK)
            total = total + weights[:, lanes]
            tangent_total = tangent_total + weighted[:, lanes]
        mixed = mixed + jnp.dot(
            weights.astype(jnp.bfloat16),
            kv_buf[slots[j], :, 2 * d : 4 * d],
            preferred_element_type=jnp.float32,
        )
        mixed_tangent = mixed_tangent + jnp.dot(
            weighted.astype(jnp.bfloat16),
            kv_buf[slots[j], :, 2 * d : 3 * d],
            preferred_element_type=jnp.float32,
        )
    inverse = 1.0 / jnp.sum(total, axis=1, keepdims=True)
    tangent_sum = jnp.sum(tangent_total, axis=1, keepdims=True)
    output = mixed[:, 0:d] * inverse
    tangent = (scale * (mixed_tangent - output * tangent_sum) + mixed[:, d : 2 * d]) * inverse
    return output.astype(jnp.bfloat16), tangent.astype(jnp.bfloat16)


def exchange_kernel(
    n, q_ref, qt_ref, k_ref, kt_ref, v_ref, vt_ref, bias_ref, o_ref, ot_ref,
    q_buf, kv_buf, xq_buf, xkv_buf, bias_buf, out_buf, xout_buf, s_buf,
    kv_send, q_send, b_send, o_send, xkv_send, xq_send, xo_send,
    kv_recv, q_recv, b_recv, o_recv, xkv_recv, xq_recv, xo_recv, greet_sem,
):
    d = HEAD_DIM
    half = n // 2
    extra = HEADS - n
    me = lax.axis_index("ctx")
    side = me // half
    place = lax.rem(me, half)
    first_host = half - extra

    def cols(head):
        return pl.ds(pl.multiple_of(head * d, d), d)

    def host(which_side, e):
        return first_host + which_side * extra + e

    row, rows, y = me // 2, n // 2, lax.rem(me, 2)
    is_inner = jnp.logical_and(row > 0, row < rows - 1)
    beside = 2 * row + 1 - y
    partner = 2 * (rows - 1 - row) + y
    along = 2 * jnp.where(row % 2 == 0, row + 1, row - 1) + y
    barrier = pltpu.get_barrier_semaphore()

    def signal(sem, target):
        pl.semaphore_signal(sem, inc=1, device_id={"ctx": target}, device_id_type=MESH)

    signal(barrier, jnp.where(is_inner, partner, beside))

    @pl.when(is_inner)
    def _():
        signal(barrier, along)

    pl.semaphore_wait(barrier, jnp.where(is_inner, 1, 2))

    def send(src, dst, send_sem, recv_sem, target):
        pltpu.make_async_remote_copy(
            src_ref=src, dst_ref=dst, send_sem=send_sem, recv_sem=recv_sem,
            device_id={"ctx": target}, device_id_type=MESH,
        ).start()

    def wait(ref, sem):
        pltpu.make_async_copy(ref, ref, sem).wait()

    packs = (k_ref, kt_ref, v_ref, vt_ref)
    pair = (qt_ref, q_ref)

    def lane(i):
        return pl.ds(i * d, d)

    def extra_send(ref, i, buf, slot, send_sem, recv_sem, which_side, e):
        target = host(which_side, e)

        @pl.when(target != me)
        def _():
            send(ref.at[:, cols(n + e)], buf.at[slot, :, lane(i)], send_sem, recv_sem, target)

        @pl.when(target == me)
        def _():
            pltpu.make_async_copy(ref.at[:, cols(n + e)], buf.at[slot, :, lane(i)], recv_sem).start()

    toward = 1 - 2 * side
    ring = [
        2 * lax.rem(row + toward * dz + rows, rows) + (1 - y if dy else y) for dz, dy in STEPS
    ]

    def main_one(i, target):
        ref = (packs + pair)[i]
        buf, send_sem, recv_sem, at = (kv_buf, kv_send, kv_recv, i) if i < 4 else (q_buf, q_send, q_recv.at[me], i - 4)
        send(ref.at[:, cols(target)], buf.at[me, :, lane(at)], send_sem, recv_sem, target)

    def extra_one(i, k, e):
        if i < 4:
            extra_send(packs[i], i, xkv_buf, me, xkv_send.at[k, e], xkv_recv, side if k else 1 - side, e)
        elif k:
            extra_send(pair[i - 4], i - 4, xq_buf, place, xq_send.at[e], xq_recv, side, e)

    def head_start(*targets):
        for i in range(HEAD_START):
            for target in targets:
                main_one(i, target)

    @pl.when(is_inner)
    def _():
        head_start(partner)
        pl.semaphore_wait(greet_sem.at[0], 1)
        signal(greet_sem.at[1], partner)
        head_start(along, beside)
        pl.semaphore_wait(greet_sem.at[1], 1)
        signal(greet_sem.at[1], along)

    @pl.when(jnp.logical_not(is_inner))
    def _():
        signal(greet_sem.at[0], beside)
        head_start(along, beside)
        pl.semaphore_wait(greet_sem.at[0], 1)
        signal(greet_sem.at[0], along)
        pl.semaphore_wait(greet_sem.at[1], 1)

    turns = [lax.rem(me + e, extra) for e in range(extra)]
    for token, i in ORDER:
        if token == "M":
            for target in ring:
                if i < HEAD_START:
                    near = functools.reduce(jnp.logical_or, [target == along, target == beside, jnp.logical_and(is_inner, target == partner)])

                    @pl.when(jnp.logical_not(near))
                    def _():
                        main_one(i, target)
                else:
                    main_one(i, target)
        elif token == "X":
            for k in (0, 1):
                for e in turns:
                    extra_one(i, k, e)
        elif token == "B":
            for target in ring:
                send(bias_ref, bias_buf.at[me], b_send, b_recv, target)
            pltpu.make_async_copy(bias_ref, bias_buf.at[me], b_recv).start()
            for i, ref in enumerate(packs):
                pltpu.make_async_copy(ref.at[:, cols(me)], kv_buf.at[me, :, lane(i)], kv_recv).start()
            for i, ref in enumerate(pair):
                pltpu.make_async_copy(ref.at[:, cols(me)], q_buf.at[me, :, lane(i)], q_recv.at[me]).start()

    def each(low, high, step):
        def run(i, carried):
            step(i)
            return carried

        lax.fori_loop(low, high, run, 0)

    wait(bias_buf, b_recv)

    is_host = jnp.logical_and(me >= first_host, me < first_host + 2 * extra)
    mine = lax.rem(me - first_host + n * extra, extra)
    outs = (o_ref, ot_ref)

    def put(buf, slot, send_sem, recv_sem, head, target):
        @pl.when(target != me)
        def _():
            for i, ref in enumerate(outs):
                send(buf.at[slot, :, lane(i)], ref.at[:, cols(head)], send_sem, recv_sem, target)

        @pl.when(target == me)
        def _():
            for i, ref in enumerate(outs):
                pltpu.make_async_copy(buf.at[slot, :, lane(i)], ref.at[:, cols(head)], recv_sem).start()

    @pl.when(is_host)
    def _():
        wait(xkv_buf, xkv_recv)
        wait(xq_buf, xq_recv)

        def step(i):
            shard = side * half + i
            output, tangent = attend(shard, i, n, xq_buf, xkv_buf, bias_buf, s_buf)
            xout_buf[i, :, 0:d] = output
            xout_buf[i, :, d : 2 * d] = tangent
            put(xout_buf, i, xo_send, xo_recv, n + mine, shard)

        each(0, half, step)

    wait(kv_buf, kv_recv)

    def order(i):
        shard = me
        for k, (at_inner, at_outer) in enumerate(zip(INNER, OUTER)):
            target = jnp.where(is_inner, (*ring, me)[at_inner], (*ring, me)[at_outer])
            shard = jnp.where(i == k, target, shard)
        return shard

    def main_step(i):
        shard = order(i)
        wait(q_buf.at[shard], q_recv.at[shard])
        output, tangent = attend(shard, shard, n, q_buf, kv_buf, bias_buf, s_buf)
        out_buf[shard, :, 0:d] = output
        out_buf[shard, :, d : 2 * d] = tangent
        put(out_buf, shard, o_send, o_recv, me, shard)

    each(0, n, main_step)

    others = pl.ds(0, n - 1)
    wait(kv_buf.at[others], kv_send)
    wait(q_buf.at[others], q_send)
    wait(bias_buf.at[others], b_send)
    for e in range(extra):
        @pl.when(host(1 - side, e) != me)
        def _():
            wait(xkv_buf.at[0], xkv_send.at[0, e])

        @pl.when(host(side, e) != me)
        def _():
            wait(xkv_buf.at[0], xkv_send.at[1, e])
            wait(xq_buf.at[0], xq_send.at[e])

    @pl.when(is_host)
    def _():
        wait(xout_buf.at[pl.ds(0, half - 1)], xo_send)

    wait(xout_buf.at[pl.ds(0, extra)], xo_recv)
    wait(out_buf.at[others], o_send)
    wait(out_buf, o_recv)


def store_kernel(a_ref, b_ref, o_ref, ot_ref, sems):
    moves = [
        pltpu.make_async_copy(a_ref, o_ref, sems.at[0]),
        pltpu.make_async_copy(b_ref, ot_ref, sems.at[1]),
    ]
    for move in moves:
        move.start()
    for move in moves:
        move.wait()


def exchanged(n, queries, query_tangents, keys, key_tangents, values, value_tangents, selection):
    rows, width = queries.shape
    half, extra, d = n // 2, HEADS - n, HEAD_DIM
    vm = pltpu.VMEM
    dma = pltpu.SemaphoreType.DMA
    reach = 2 * REACH + 1
    bf = jnp.bfloat16
    landed = pl.pallas_call(
        functools.partial(exchange_kernel, n),
        out_shape=[vm((rows, width), bf)] * 2,
        in_specs=[pl.BlockSpec(memory_space=pl.ANY)] * 7,
        out_specs=[pl.BlockSpec(memory_space=vm)] * 2,
        scratch_shapes=[
            vm((n, rows, 2 * d), bf),
            vm((n, rows, 4 * d), bf),
            vm((half, rows, 2 * d), bf),
            vm((n, rows, 4 * d), bf),
            vm((n,) + selection.shape, jnp.int32),
            vm((n, rows, 2 * d), bf),
            vm((half, rows, 2 * d), bf),
            vm((reach, rows, rows), jnp.float32),
            dma, dma, dma, dma, dma((2, extra)), dma((extra,)), dma,
            dma, dma((n,)), dma, dma, dma, dma, dma,
            pltpu.SemaphoreType.REGULAR((2,)),
        ],
        compiler_params=pltpu.CompilerParams(
            collective_id=0, has_side_effects=True, vmem_limit_bytes=67_043_328 - 4 * rows * width - 131_072
        ),
        name="exchange",
    )(queries, query_tangents, keys, key_tangents, values, value_tangents, selection)
    return pl.pallas_call(
        store_kernel,
        out_shape=[jax.ShapeDtypeStruct((rows, width), bf)] * 2,
        in_specs=[pl.BlockSpec(memory_space=vm)] * 2,
        out_specs=[pl.BlockSpec(memory_space=pl.ANY)] * 2,
        scratch_shapes=[dma((2,))],
        name="store",
    )(*[pltpu.with_memory_space_constraint(x, vm) for x in landed])


def solution(mesh):
    n = mesh.shape["ctx"]
    covered = n == 2 * REACH + 2 and n < HEADS and 2 * (HEADS - n) <= n
    placed = (
        P("ctx", "head"),
        P("ctx", "head"),
        P("ctx", "head"),
        P("ctx", "head"),
        P("ctx", "head"),
        P("ctx", "head"),
        P("ctx", None),
    )
    return jax.shard_map(
        functools.partial(exchanged, n) if covered else body,
        mesh=mesh,
        in_specs=placed,
        out_specs=(P("ctx", "head"), P("ctx", "head")),
        check_vma=False,
    )
```

```python
import functools

import jax
import jax.numpy as jnp
from jax import lax
from jax.sharding import PartitionSpec as P
from jax.experimental import pallas as pl
from jax.experimental.pallas import tpu as pltpu

HEADS = 10
HEAD_DIM = 128
BLK = 128
REACH = 3


big_negative = -1e30


def from_behind(array, axis, by):
    devices = lax.axis_size(axis)
    return lax.ppermute(array, axis, [(i, (i + by) % devices) for i in range(devices)])


def heads_view(flat_array):
    return flat_array.reshape(flat_array.shape[0], HEADS, HEAD_DIM)


def tile_update(accumulators, query_pieces, key_pieces):
    score_scale = HEAD_DIM ** (-0.5)
    query_block, query_tangent = query_pieces
    key_block, key_tangent, value_block, value_tangent = key_pieces
    running, weight_total, tangent_total, mixed_sum, mixed_tangent = accumulators
    scores = (
        jnp.einsum("qhd,khd->qhk", query_block, key_block, preferred_element_type=jnp.float32)
        * score_scale
    )
    score_tangents = (
        jnp.einsum("qhd,khd->qhk", query_tangent, key_block, preferred_element_type=jnp.float32)
        + jnp.einsum("qhd,khd->qhk", query_block, key_tangent, preferred_element_type=jnp.float32)
    ) * score_scale
    highest = jnp.maximum(running, scores.max(axis=2))
    factor = jnp.exp(running - highest)
    weights = jnp.exp(scores - highest[:, :, None])
    weighted = weights * score_tangents
    weight_total = factor * weight_total + weights.sum(axis=2)
    tangent_total = factor * tangent_total + weighted.sum(axis=2)
    rounded_weights = weights.astype(jnp.bfloat16)
    rounded_tangent = weighted.astype(jnp.bfloat16)
    mixed_sum = factor[:, :, None] * mixed_sum + jnp.einsum(
        "qhk,khd->qhd", rounded_weights, value_block, preferred_element_type=jnp.float32
    )
    mixed_tangent = (
        factor[:, :, None] * mixed_tangent
        + jnp.einsum(
            "qhk,khd->qhd", rounded_tangent, value_block, preferred_element_type=jnp.float32
        )
        + jnp.einsum(
            "qhk,khd->qhd", rounded_weights, value_tangent, preferred_element_type=jnp.float32
        )
    )
    return (highest, weight_total, tangent_total, mixed_sum, mixed_tangent)


def sweep(accumulators, query_pair, chosen_rows, key_pack, column_base):
    per_device = chosen_rows.shape[0]

    def visit(tile_index, carried):
        query_index = tile_index // per_device
        key_index = tile_index % per_device
        picked = chosen_rows[query_index, column_base + key_index] != 0

        def apply(carried_state):
            first_row = query_index * BLK
            pieces = tuple(
                (
                    lax.dynamic_slice_in_dim(full_array, first_row, BLK, 0)
                    for full_array in carried_state
                )
            )
            query_pieces = tuple(
                (
                    lax.dynamic_slice_in_dim(full_array, first_row, BLK, 0)
                    for full_array in query_pair
                )
            )
            key_pieces = tuple(
                (
                    lax.dynamic_slice_in_dim(full_array, key_index * BLK, BLK, 0)
                    for full_array in key_pack
                )
            )
            updated = tile_update(pieces, query_pieces, key_pieces)
            return tuple(
                (
                    lax.dynamic_update_slice_in_dim(full_array, new_piece, first_row, 0)
                    for full_array, new_piece in zip(carried_state, updated)
                )
            )

        return lax.cond(picked, apply, lambda unchanged: unchanged, carried)

    return lax.fori_loop(0, per_device * per_device, visit, tuple(accumulators))


def finish(accumulators):
    running, weight_total, tangent_total, mixed_sum, mixed_tangent = accumulators
    token_count = mixed_sum.shape[0]
    output = mixed_sum / weight_total[:, :, None]
    tangent = (mixed_tangent - output * tangent_total[:, :, None]) / weight_total[:, :, None]
    return (
        output.reshape(token_count, HEADS * HEAD_DIM).astype(jnp.bfloat16),
        tangent.reshape(token_count, HEADS * HEAD_DIM).astype(jnp.bfloat16),
    )


def body(queries, query_tangents, keys, key_tangents, values, value_tangents, selection):
    token_count = queries.shape[0]
    per_device = token_count // BLK
    query_pair = (heads_view(queries), heads_view(query_tangents))
    key_pack = (
        heads_view(keys),
        heads_view(key_tangents),
        heads_view(values),
        heads_view(value_tangents),
    )
    initial = (
        jnp.full((token_count, HEADS), big_negative, jnp.float32),
        jnp.zeros((token_count, HEADS), jnp.float32),
        jnp.zeros((token_count, HEADS), jnp.float32),
        jnp.zeros((token_count, HEADS, HEAD_DIM), jnp.float32),
        jnp.zeros((token_count, HEADS, HEAD_DIM), jnp.float32),
    )
    at_home = sweep(initial, query_pair, selection, key_pack, REACH * per_device)
    accumulators = at_home
    rising = key_pack
    falling = key_pack
    for offset in range(1, REACH + 1):
        rising = from_behind((rising[0], rising[1], rising[2], rising[3]), "ctx", -1)
        accumulators = sweep(
            accumulators, query_pair, selection, rising, (REACH + offset) * per_device
        )
        falling = from_behind((falling[0], falling[1], falling[2], falling[3]), "ctx", 1)
        accumulators = sweep(
            accumulators, query_pair, selection, falling, (REACH - offset) * per_device
        )
    return finish(accumulators)


ORDER = [('M', 0), ('B', 0), ('X', 0), ('X', 1), ('X', 2), ('X', 3), ('X', 4), ('X', 5), ('M', 1), ('M', 2), ('M', 3), ('M', 4), ('M', 5)]
HEAD_START = 4
STEPS = [(2, 0), (2, 1), (1, 1), (1, 0), (3, 1), (3, 0), (0, 1)]
INNER = [5, 4, 6, 7, 0, 1, 2, 3]
OUTER = [3, 2, 6, 7, 0, 1, 4, 5]
LOG2E = 1.4426950408889634
MESH = pl.DeviceIdType.MESH


def attend(shard, q_slot, n, q_buf, kv_buf, bias_buf, s_buf):
    scale = HEAD_DIM ** (-0.5)
    factor = scale * LOG2E
    width = 2 * REACH + 1
    d = HEAD_DIM
    both = q_buf[q_slot]
    query = q_buf[q_slot, :, d : 2 * d]
    rows = both.shape[0]
    per_device = rows // BLK
    bias = jnp.where(bias_buf[shard] != 0, 0.0, big_negative)
    dims = (((1,), (1,)), ((), ()))
    slots = [lax.rem(shard + n - REACH + j, n) for j in range(width)]
    high = [None] * per_device
    for j in range(width):
        scores = lax.dot_general(
            query, kv_buf[slots[j], :, 0:d], dims, preferred_element_type=jnp.float32
        )
        for r in range(per_device):
            for k in range(per_device):
                column = j * per_device + k
                there = (slice(r * BLK, (r + 1) * BLK), slice(k * BLK, (k + 1) * BLK))
                masked = scores[there] * factor + bias[r : r + 1, column : column + 1]
                s_buf[(j,) + there] = masked
                high[r] = masked if high[r] is None else jnp.maximum(high[r], masked)
    peak = jnp.concatenate([jnp.max(h, axis=1, keepdims=True) for h in high], axis=0)
    total = jnp.zeros((rows, BLK), jnp.float32)
    tangent_total = jnp.zeros((rows, BLK), jnp.float32)
    mixed = jnp.zeros((rows, 2 * d), jnp.float32)
    mixed_tangent = jnp.zeros((rows, d), jnp.float32)
    for j in range(width):
        tangents = lax.dot_general(
            both, kv_buf[slots[j], :, 0 : 2 * d], dims, preferred_element_type=jnp.float32
        )
        weights = jnp.exp2(s_buf[j] - peak)
        weighted = weights * tangents
        for k in range(per_device):
            lanes = slice(k * BLK, (k + 1) * BLK)
            total = total + weights[:, lanes]
            tangent_total = tangent_total + weighted[:, lanes]
        mixed = mixed + jnp.dot(
            weights.astype(jnp.bfloat16),
            kv_buf[slots[j], :, 2 * d : 4 * d],
            preferred_element_type=jnp.float32,
        )
        mixed_tangent = mixed_tangent + jnp.dot(
            weighted.astype(jnp.bfloat16),
            kv_buf[slots[j], :, 2 * d : 3 * d],
            preferred_element_type=jnp.float32,
        )
    inverse = 1.0 / jnp.sum(total, axis=1, keepdims=True)
    tangent_sum = jnp.sum(tangent_total, axis=1, keepdims=True)
    output = mixed[:, 0:d] * inverse
    tangent = (scale * (mixed_tangent - output * tangent_sum) + mixed[:, d : 2 * d]) * inverse
    return output.astype(jnp.bfloat16), tangent.astype(jnp.bfloat16)


def exchange_kernel(
    n, q_ref, qt_ref, k_ref, kt_ref, v_ref, vt_ref, bias_ref, o_ref, ot_ref,
    q_buf, kv_buf, xq_buf, xkv_buf, bias_buf, out_buf, xout_buf, s_buf,
    kv_send, q_send, b_send, o_send, xkv_send, xq_send, xo_send,
    kv_recv, q_recv, b_recv, o_recv, xkv_recv, xq_recv, xo_recv, greet_sem,
):
    d = HEAD_DIM
    half = n // 2
    extra = HEADS - n
    me = lax.axis_index("ctx")
    side = me // half
    place = lax.rem(me, half)
    first_host = half - extra

    def cols(head):
        return pl.ds(pl.multiple_of(head * d, d), d)

    def host(which_side, e):
        return first_host + which_side * extra + e

    row, rows, y = me // 2, n // 2, lax.rem(me, 2)
    is_inner = jnp.logical_and(row > 0, row < rows - 1)
    beside = 2 * row + 1 - y
    partner = 2 * (rows - 1 - row) + y
    along = 2 * jnp.where(row % 2 == 0, row + 1, row - 1) + y
    barrier = pltpu.get_barrier_semaphore()

    def signal(sem, target):
        pl.semaphore_signal(sem, inc=1, device_id={"ctx": target}, device_id_type=MESH)

    signal(barrier, jnp.where(is_inner, partner, beside))

    @pl.when(is_inner)
    def _():
        signal(barrier, along)

    pl.semaphore_wait(barrier, jnp.where(is_inner, 1, 2))

    def send(src, dst, send_sem, recv_sem, target):
        pltpu.make_async_remote_copy(
            src_ref=src, dst_ref=dst, send_sem=send_sem, recv_sem=recv_sem,
            device_id={"ctx": target}, device_id_type=MESH,
        ).start()

    def wait(ref, sem):
        pltpu.make_async_copy(ref, ref, sem).wait()

    packs = (k_ref, kt_ref, v_ref, vt_ref)
    pair = (qt_ref, q_ref)

    def lane(i):
        return pl.ds(i * d, d)

    def extra_send(ref, i, buf, slot, send_sem, recv_sem, which_side, e):
        target = host(which_side, e)

        @pl.when(target != me)
        def _():
            send(ref.at[:, cols(n + e)], buf.at[slot, :, lane(i)], send_sem, recv_sem, target)

        @pl.when(target == me)
        def _():
            pltpu.make_async_copy(ref.at[:, cols(n + e)], buf.at[slot, :, lane(i)], recv_sem).start()

    toward = 1 - 2 * side
    ring = [
        2 * lax.rem(row + toward * dz + rows, rows) + (1 - y if dy else y) for dz, dy in STEPS
    ]

    def main_one(i, target):
        ref = (packs + pair)[i]
        buf, send_sem, recv_sem, at = (kv_buf, kv_send, kv_recv, i) if i < 4 else (q_buf, q_send, q_recv.at[me], i - 4)
        send(ref.at[:, cols(target)], buf.at[me, :, lane(at)], send_sem, recv_sem, target)

    def extra_one(i, k, e):
        if i < 4:
            extra_send(packs[i], i, xkv_buf, me, xkv_send.at[k, e], xkv_recv, side if k else 1 - side, e)
        elif k:
            extra_send(pair[i - 4], i - 4, xq_buf, place, xq_send.at[e], xq_recv, side, e)

    def head_start(*targets):
        for i in range(HEAD_START):
            for target in targets:
                main_one(i, target)

    @pl.when(is_inner)
    def _():
        head_start(partner)
        pl.semaphore_wait(greet_sem.at[0], 1)
        signal(greet_sem.at[1], partner)
        head_start(along, beside)
        pl.semaphore_wait(greet_sem.at[1], 1)
        signal(greet_sem.at[1], along)

    @pl.when(jnp.logical_not(is_inner))
    def _():
        signal(greet_sem.at[0], beside)
        head_start(along, beside)
        pl.semaphore_wait(greet_sem.at[0], 1)
        signal(greet_sem.at[0], along)
        pl.semaphore_wait(greet_sem.at[1], 1)

    turns = [lax.rem(me + e, extra) for e in range(extra)]
    for token, i in ORDER:
        if token == "M":
            for target in ring:
                if i < HEAD_START:
                    near = functools.reduce(jnp.logical_or, [target == along, target == beside, jnp.logical_and(is_inner, target == partner)])

                    @pl.when(jnp.logical_not(near))
                    def _():
                        main_one(i, target)
                else:
                    main_one(i, target)
        elif token == "X":
            for k in (0, 1):
                for e in turns:
                    extra_one(i, k, e)
        elif token == "B":
            for target in ring:
                send(bias_ref, bias_buf.at[me], b_send, b_recv, target)
            pltpu.make_async_copy(bias_ref, bias_buf.at[me], b_recv).start()
            for i, ref in enumerate(packs):
                pltpu.make_async_copy(ref.at[:, cols(me)], kv_buf.at[me, :, lane(i)], kv_recv).start()
            for i, ref in enumerate(pair):
                pltpu.make_async_copy(ref.at[:, cols(me)], q_buf.at[me, :, lane(i)], q_recv.at[me]).start()

    def each(low, high, step):
        def run(i, carried):
            step(i)
            return carried

        lax.fori_loop(low, high, run, 0)

    wait(bias_buf, b_recv)

    is_host = jnp.logical_and(me >= first_host, me < first_host + 2 * extra)
    mine = lax.rem(me - first_host + n * extra, extra)
    outs = (o_ref, ot_ref)

    def put(buf, slot, send_sem, recv_sem, head, target):
        @pl.when(target != me)
        def _():
            for i, ref in enumerate(outs):
                send(buf.at[slot, :, lane(i)], ref.at[:, cols(head)], send_sem, recv_sem, target)

        @pl.when(target == me)
        def _():
            for i, ref in enumerate(outs):
                pltpu.make_async_copy(buf.at[slot, :, lane(i)], ref.at[:, cols(head)], recv_sem).start()

    @pl.when(is_host)
    def _():
        wait(xkv_buf, xkv_recv)
        wait(xq_buf, xq_recv)

        def step(i):
            shard = side * half + i
            output, tangent = attend(shard, i, n, xq_buf, xkv_buf, bias_buf, s_buf)
            xout_buf[i, :, 0:d] = output
            xout_buf[i, :, d : 2 * d] = tangent
            put(xout_buf, i, xo_send, xo_recv, n + mine, shard)

        each(0, half, step)

    wait(kv_buf, kv_recv)

    def order(i):
        shard = me
        for k, (at_inner, at_outer) in enumerate(zip(INNER, OUTER)):
            target = jnp.where(is_inner, (*ring, me)[at_inner], (*ring, me)[at_outer])
            shard = jnp.where(i == k, target, shard)
        return shard

    def main_step(i):
        shard = order(i)
        wait(q_buf.at[shard], q_recv.at[shard])
        output, tangent = attend(shard, shard, n, q_buf, kv_buf, bias_buf, s_buf)
        out_buf[shard, :, 0:d] = output
        out_buf[shard, :, d : 2 * d] = tangent
        put(out_buf, shard, o_send, o_recv, me, shard)

    each(0, n, main_step)

    others = pl.ds(0, n - 1)
    wait(kv_buf.at[others], kv_send)
    wait(q_buf.at[others], q_send)
    wait(bias_buf.at[others], b_send)
    for e in range(extra):
        @pl.when(host(1 - side, e) != me)
        def _():
            wait(xkv_buf.at[0], xkv_send.at[0, e])

        @pl.when(host(side, e) != me)
        def _():
            wait(xkv_buf.at[0], xkv_send.at[1, e])
            wait(xq_buf.at[0], xq_send.at[e])

    @pl.when(is_host)
    def _():
        wait(xout_buf.at[pl.ds(0, half - 1)], xo_send)

    wait(xout_buf.at[pl.ds(0, extra)], xo_recv)
    wait(out_buf.at[others], o_send)
    wait(out_buf, o_recv)


def store_kernel(a_ref, b_ref, o_ref, ot_ref, sems):
    moves = [
        pltpu.make_async_copy(a_ref, o_ref, sems.at[0]),
        pltpu.make_async_copy(b_ref, ot_ref, sems.at[1]),
    ]
    for move in moves:
        move.start()
    for move in moves:
        move.wait()


def exchanged(n, queries, query_tangents, keys, key_tangents, values, value_tangents, selection):
    rows, width = queries.shape
    half, extra, d = n // 2, HEADS - n, HEAD_DIM
    vm = pltpu.VMEM
    dma = pltpu.SemaphoreType.DMA
    reach = 2 * REACH + 1
    bf = jnp.bfloat16
    landed = pl.pallas_call(
        functools.partial(exchange_kernel, n),
        out_shape=[vm((rows, width), bf)] * 2,
        in_specs=[pl.BlockSpec(memory_space=pl.ANY)] * 7,
        out_specs=[pl.BlockSpec(memory_space=vm)] * 2,
        scratch_shapes=[
            vm((n, rows, 2 * d), bf),
            vm((n, rows, 4 * d), bf),
            vm((half, rows, 2 * d), bf),
            vm((n, rows, 4 * d), bf),
            vm((n,) + selection.shape, jnp.int32),
            vm((n, rows, 2 * d), bf),
            vm((half, rows, 2 * d), bf),
            vm((reach, rows, rows), jnp.float32),
            dma, dma, dma, dma, dma((2, extra)), dma((extra,)), dma,
            dma, dma((n,)), dma, dma, dma, dma, dma,
            pltpu.SemaphoreType.REGULAR((2,)),
        ],
        compiler_params=pltpu.CompilerParams(
            collective_id=0, has_side_effects=True, vmem_limit_bytes=67_043_328 - 4 * rows * width - 131_072
        ),
        name="exchange",
    )(queries, query_tangents, keys, key_tangents, values, value_tangents, selection)
    return pl.pallas_call(
        store_kernel,
        out_shape=[jax.ShapeDtypeStruct((rows, width), bf)] * 2,
        in_specs=[pl.BlockSpec(memory_space=vm)] * 2,
        out_specs=[pl.BlockSpec(memory_space=pl.ANY)] * 2,
        scratch_shapes=[dma((2,))],
        name="store",
    )(*[pltpu.with_memory_space_constraint(x, vm) for x in landed])


def solution(mesh):
    n = mesh.shape["ctx"]
    covered = n == 2 * REACH + 2 and n < HEADS and 2 * (HEADS - n) <= n
    placed = (
        P("ctx", "head"),
        P("ctx", "head"),
        P("ctx", "head"),
        P("ctx", "head"),
        P("ctx", "head"),
        P("ctx", "head"),
        P("ctx", None),
    )
    return jax.shard_map(
        functools.partial(exchanged, n) if covered else body,
        mesh=mesh,
        in_specs=placed,
        out_specs=(P("ctx", "head"), P("ctx", "head")),
        check_vma=False,
    )
```

```python
import functools

import jax
import jax.numpy as jnp
from jax import lax
from jax.sharding import PartitionSpec as P
from jax.experimental import pallas as pl
from jax.experimental.pallas import tpu as pltpu

HEADS = 10
HEAD_DIM = 128
BLK = 128
REACH = 3


big_negative = -1e30


def from_behind(array, axis, by):
    devices = lax.axis_size(axis)
    return lax.ppermute(array, axis, [(i, (i + by) % devices) for i in range(devices)])


def heads_view(flat_array):
    return flat_array.reshape(flat_array.shape[0], HEADS, HEAD_DIM)


def tile_update(accumulators, query_pieces, key_pieces):
    score_scale = HEAD_DIM ** (-0.5)
    query_block, query_tangent = query_pieces
    key_block, key_tangent, value_block, value_tangent = key_pieces
    running, weight_total, tangent_total, mixed_sum, mixed_tangent = accumulators
    scores = (
        jnp.einsum("qhd,khd->qhk", query_block, key_block, preferred_element_type=jnp.float32)
        * score_scale
    )
    score_tangents = (
        jnp.einsum("qhd,khd->qhk", query_tangent, key_block, preferred_element_type=jnp.float32)
        + jnp.einsum("qhd,khd->qhk", query_block, key_tangent, preferred_element_type=jnp.float32)
    ) * score_scale
    highest = jnp.maximum(running, scores.max(axis=2))
    factor = jnp.exp(running - highest)
    weights = jnp.exp(scores - highest[:, :, None])
    weighted = weights * score_tangents
    weight_total = factor * weight_total + weights.sum(axis=2)
    tangent_total = factor * tangent_total + weighted.sum(axis=2)
    rounded_weights = weights.astype(jnp.bfloat16)
    rounded_tangent = weighted.astype(jnp.bfloat16)
    mixed_sum = factor[:, :, None] * mixed_sum + jnp.einsum(
        "qhk,khd->qhd", rounded_weights, value_block, preferred_element_type=jnp.float32
    )
    mixed_tangent = (
        factor[:, :, None] * mixed_tangent
        + jnp.einsum(
            "qhk,khd->qhd", rounded_tangent, value_block, preferred_element_type=jnp.float32
        )
        + jnp.einsum(
            "qhk,khd->qhd", rounded_weights, value_tangent, preferred_element_type=jnp.float32
        )
    )
    return (highest, weight_total, tangent_total, mixed_sum, mixed_tangent)


def sweep(accumulators, query_pair, chosen_rows, key_pack, column_base):
    per_device = chosen_rows.shape[0]

    def visit(tile_index, carried):
        query_index = tile_index // per_device
        key_index = tile_index % per_device
        picked = chosen_rows[query_index, column_base + key_index] != 0

        def apply(carried_state):
            first_row = query_index * BLK
            pieces = tuple(
                (
                    lax.dynamic_slice_in_dim(full_array, first_row, BLK, 0)
                    for full_array in carried_state
                )
            )
            query_pieces = tuple(
                (
                    lax.dynamic_slice_in_dim(full_array, first_row, BLK, 0)
                    for full_array in query_pair
                )
            )
            key_pieces = tuple(
                (
                    lax.dynamic_slice_in_dim(full_array, key_index * BLK, BLK, 0)
                    for full_array in key_pack
                )
            )
            updated = tile_update(pieces, query_pieces, key_pieces)
            return tuple(
                (
                    lax.dynamic_update_slice_in_dim(full_array, new_piece, first_row, 0)
                    for full_array, new_piece in zip(carried_state, updated)
                )
            )

        return lax.cond(picked, apply, lambda unchanged: unchanged, carried)

    return lax.fori_loop(0, per_device * per_device, visit, tuple(accumulators))


def finish(accumulators):
    running, weight_total, tangent_total, mixed_sum, mixed_tangent = accumulators
    token_count = mixed_sum.shape[0]
    output = mixed_sum / weight_total[:, :, None]
    tangent = (mixed_tangent - output * tangent_total[:, :, None]) / weight_total[:, :, None]
    return (
        output.reshape(token_count, HEADS * HEAD_DIM).astype(jnp.bfloat16),
        tangent.reshape(token_count, HEADS * HEAD_DIM).astype(jnp.bfloat16),
    )


def body(queries, query_tangents, keys, key_tangents, values, value_tangents, selection):
    token_count = queries.shape[0]
    per_device = token_count // BLK
    query_pair = (heads_view(queries), heads_view(query_tangents))
    key_pack = (
        heads_view(keys),
        heads_view(key_tangents),
        heads_view(values),
        heads_view(value_tangents),
    )
    initial = (
        jnp.full((token_count, HEADS), big_negative, jnp.float32),
        jnp.zeros((token_count, HEADS), jnp.float32),
        jnp.zeros((token_count, HEADS), jnp.float32),
        jnp.zeros((token_count, HEADS, HEAD_DIM), jnp.float32),
        jnp.zeros((token_count, HEADS, HEAD_DIM), jnp.float32),
    )
    at_home = sweep(initial, query_pair, selection, key_pack, REACH * per_device)
    accumulators = at_home
    rising = key_pack
    falling = key_pack
    for offset in range(1, REACH + 1):
        rising = from_behind((rising[0], rising[1], rising[2], rising[3]), "ctx", -1)
        accumulators = sweep(
            accumulators, query_pair, selection, rising, (REACH + offset) * per_device
        )
        falling = from_behind((falling[0], falling[1], falling[2], falling[3]), "ctx", 1)
        accumulators = sweep(
            accumulators, query_pair, selection, falling, (REACH - offset) * per_device
        )
    return finish(accumulators)


ORDER = [('M', 0), ('B', 0), ('X', 0), ('X', 1), ('X', 2), ('X', 3), ('X', 4), ('X', 5), ('M', 1), ('M', 2), ('M', 3), ('M', 4), ('M', 5)]
HEAD_START = 3
STEPS = [(2, 0), (2, 1), (1, 1), (1, 0), (3, 1), (3, 0), (0, 1)]
INNER = [0, 1, 5, 4, 6, 7, 2, 3]
OUTER = [3, 2, 6, 7, 0, 1, 4, 5]
LOG2E = 1.4426950408889634
MESH = pl.DeviceIdType.MESH


def attend(shard, q_slot, n, q_buf, kv_buf, bias_buf, s_buf):
    scale = HEAD_DIM ** (-0.5)
    factor = scale * LOG2E
    width = 2 * REACH + 1
    d = HEAD_DIM
    both = q_buf[q_slot]
    query = q_buf[q_slot, :, d : 2 * d]
    rows = both.shape[0]
    per_device = rows // BLK
    bias = jnp.where(bias_buf[shard] != 0, 0.0, big_negative)
    dims = (((1,), (1,)), ((), ()))
    slots = [lax.rem(shard + n - REACH + j, n) for j in range(width)]
    high = [None] * per_device
    for j in range(width):
        scores = lax.dot_general(
            query, kv_buf[slots[j], :, 0:d], dims, preferred_element_type=jnp.float32
        )
        for r in range(per_device):
            for k in range(per_device):
                column = j * per_device + k
                there = (slice(r * BLK, (r + 1) * BLK), slice(k * BLK, (k + 1) * BLK))
                masked = scores[there] * factor + bias[r : r + 1, column : column + 1]
                s_buf[(j,) + there] = masked
                high[r] = masked if high[r] is None else jnp.maximum(high[r], masked)
    peak = jnp.concatenate([jnp.max(h, axis=1, keepdims=True) for h in high], axis=0)
    total = jnp.zeros((rows, BLK), jnp.float32)
    tangent_total = jnp.zeros((rows, BLK), jnp.float32)
    mixed = jnp.zeros((rows, 2 * d), jnp.float32)
    mixed_tangent = jnp.zeros((rows, d), jnp.float32)
    for j in range(width):
        tangents = lax.dot_general(
            both, kv_buf[slots[j], :, 0 : 2 * d], dims, preferred_element_type=jnp.float32
        )
        weights = jnp.exp2(s_buf[j] - peak)
        weighted = weights * tangents
        for k in range(per_device):
            lanes = slice(k * BLK, (k + 1) * BLK)
            total = total + weights[:, lanes]
            tangent_total = tangent_total + weighted[:, lanes]
        mixed = mixed + jnp.dot(
            weights.astype(jnp.bfloat16),
            kv_buf[slots[j], :, 2 * d : 4 * d],
            preferred_element_type=jnp.float32,
        )
        mixed_tangent = mixed_tangent + jnp.dot(
            weighted.astype(jnp.bfloat16),
            kv_buf[slots[j], :, 2 * d : 3 * d],
            preferred_element_type=jnp.float32,
        )
    inverse = 1.0 / jnp.sum(total, axis=1, keepdims=True)
    tangent_sum = jnp.sum(tangent_total, axis=1, keepdims=True)
    output = mixed[:, 0:d] * inverse
    tangent = (scale * (mixed_tangent - output * tangent_sum) + mixed[:, d : 2 * d]) * inverse
    return output.astype(jnp.bfloat16), tangent.astype(jnp.bfloat16)


def exchange_kernel(
    n, q_ref, qt_ref, k_ref, kt_ref, v_ref, vt_ref, bias_ref, o_ref, ot_ref,
    q_buf, kv_buf, xq_buf, xkv_buf, bias_buf, out_buf, xout_buf, s_buf,
    kv_send, q_send, b_send, o_send, xkv_send, xq_send, xo_send,
    kv_recv, q_recv, b_recv, o_recv, xkv_recv, xq_recv, xo_recv, greet_sem,
):
    d = HEAD_DIM
    half = n // 2
    extra = HEADS - n
    me = lax.axis_index("ctx")
    side = me // half
    place = lax.rem(me, half)
    first_host = half - extra

    def cols(head):
        return pl.ds(pl.multiple_of(head * d, d), d)

    def host(which_side, e):
        return first_host + which_side * extra + e

    row, rows, y = me // 2, n // 2, lax.rem(me, 2)
    is_inner = jnp.logical_and(row > 0, row < rows - 1)
    beside = 2 * row + 1 - y
    partner = 2 * (rows - 1 - row) + y
    along = 2 * jnp.where(row % 2 == 0, row + 1, row - 1) + y
    barrier = pltpu.get_barrier_semaphore()

    def signal(sem, target):
        pl.semaphore_signal(sem, inc=1, device_id={"ctx": target}, device_id_type=MESH)

    signal(barrier, jnp.where(is_inner, partner, beside))

    @pl.when(is_inner)
    def _():
        signal(barrier, along)

    pl.semaphore_wait(barrier, jnp.where(is_inner, 1, 2))

    def send(src, dst, send_sem, recv_sem, target):
        pltpu.make_async_remote_copy(
            src_ref=src, dst_ref=dst, send_sem=send_sem, recv_sem=recv_sem,
            device_id={"ctx": target}, device_id_type=MESH,
        ).start()

    def wait(ref, sem):
        pltpu.make_async_copy(ref, ref, sem).wait()

    packs = (k_ref, kt_ref, v_ref, vt_ref)
    pair = (qt_ref, q_ref)

    def lane(i):
        return pl.ds(i * d, d)

    def extra_send(ref, i, buf, slot, send_sem, recv_sem, which_side, e):
        target = host(which_side, e)

        @pl.when(target != me)
        def _():
            send(ref.at[:, cols(n + e)], buf.at[slot, :, lane(i)], send_sem, recv_sem, target)

        @pl.when(target == me)
        def _():
            pltpu.make_async_copy(ref.at[:, cols(n + e)], buf.at[slot, :, lane(i)], recv_sem).start()

    toward = 1 - 2 * side
    ring = [
        2 * lax.rem(row + toward * dz + rows, rows) + (1 - y if dy else y) for dz, dy in STEPS
    ]

    def main_one(i, target):
        ref = (packs + pair)[i]
        buf, send_sem, recv_sem, at = (kv_buf, kv_send, kv_recv, i) if i < 4 else (q_buf, q_send, q_recv.at[me], i - 4)
        send(ref.at[:, cols(target)], buf.at[me, :, lane(at)], send_sem, recv_sem, target)

    def extra_one(i, k, e):
        if i < 4:
            extra_send(packs[i], i, xkv_buf, me, xkv_send.at[k, e], xkv_recv, side if k else 1 - side, e)
        elif k:
            extra_send(pair[i - 4], i - 4, xq_buf, place, xq_send.at[e], xq_recv, side, e)

    def head_start(*targets):
        for i in range(HEAD_START):
            for target in targets:
                main_one(i, target)

    @pl.when(is_inner)
    def _():
        head_start(partner)
        pl.semaphore_wait(greet_sem.at[0], 1)
        signal(greet_sem.at[1], partner)
        head_start(along, beside)
        pl.semaphore_wait(greet_sem.at[1], 1)
        signal(greet_sem.at[1], along)

    @pl.when(jnp.logical_not(is_inner))
    def _():
        signal(greet_sem.at[0], beside)
        head_start(along, beside)
        pl.semaphore_wait(greet_sem.at[0], 1)
        signal(greet_sem.at[0], along)
        pl.semaphore_wait(greet_sem.at[1], 1)

    turns = [lax.rem(me + e, extra) for e in range(extra)]
    for token, i in ORDER:
        if token == "M":
            for target in ring:
                if i < HEAD_START:
                    near = functools.reduce(jnp.logical_or, [target == along, target == beside, jnp.logical_and(is_inner, target == partner)])

                    @pl.when(jnp.logical_not(near))
                    def _():
                        main_one(i, target)
                else:
                    main_one(i, target)
        elif token == "X":
            for k in (0, 1):
                for e in turns:
                    extra_one(i, k, e)
        elif token == "B":
            for target in ring:
                send(bias_ref, bias_buf.at[me], b_send, b_recv, target)
            pltpu.make_async_copy(bias_ref, bias_buf.at[me], b_recv).start()
            for i, ref in enumerate(packs):
                pltpu.make_async_copy(ref.at[:, cols(me)], kv_buf.at[me, :, lane(i)], kv_recv).start()
            for i, ref in enumerate(pair):
                pltpu.make_async_copy(ref.at[:, cols(me)], q_buf.at[me, :, lane(i)], q_recv.at[me]).start()

    def each(low, high, step):
        def run(i, carried):
            step(i)
            return carried

        lax.fori_loop(low, high, run, 0)

    wait(bias_buf, b_recv)

    is_host = jnp.logical_and(me >= first_host, me < first_host + 2 * extra)
    mine = lax.rem(me - first_host + n * extra, extra)
    outs = (o_ref, ot_ref)

    def put(buf, slot, send_sem, recv_sem, head, target):
        @pl.when(target != me)
        def _():
            for i, ref in enumerate(outs):
                send(buf.at[slot, :, lane(i)], ref.at[:, cols(head)], send_sem, recv_sem, target)

        @pl.when(target == me)
        def _():
            for i, ref in enumerate(outs):
                pltpu.make_async_copy(buf.at[slot, :, lane(i)], ref.at[:, cols(head)], recv_sem).start()

    @pl.when(is_host)
    def _():
        wait(xkv_buf, xkv_recv)
        wait(xq_buf, xq_recv)

        def step(i):
            shard = side * half + i
            output, tangent = attend(shard, i, n, xq_buf, xkv_buf, bias_buf, s_buf)
            xout_buf[i, :, 0:d] = output
            xout_buf[i, :, d : 2 * d] = tangent
            put(xout_buf, i, xo_send, xo_recv, n + mine, shard)

        each(0, half, step)

    wait(kv_buf, kv_recv)

    def order(i):
        shard = me
        for k, (at_inner, at_outer) in enumerate(zip(INNER, OUTER)):
            target = jnp.where(is_inner, (*ring, me)[at_inner], (*ring, me)[at_outer])
            shard = jnp.where(i == k, target, shard)
        return shard

    def main_step(i):
        shard = order(i)
        wait(q_buf.at[shard], q_recv.at[shard])
        output, tangent = attend(shard, shard, n, q_buf, kv_buf, bias_buf, s_buf)
        out_buf[shard, :, 0:d] = output
        out_buf[shard, :, d : 2 * d] = tangent
        put(out_buf, shard, o_send, o_recv, me, shard)

    each(0, n, main_step)

    others = pl.ds(0, n - 1)
    wait(kv_buf.at[others], kv_send)
    wait(q_buf.at[others], q_send)
    wait(bias_buf.at[others], b_send)
    for e in range(extra):
        @pl.when(host(1 - side, e) != me)
        def _():
            wait(xkv_buf.at[0], xkv_send.at[0, e])

        @pl.when(host(side, e) != me)
        def _():
            wait(xkv_buf.at[0], xkv_send.at[1, e])
            wait(xq_buf.at[0], xq_send.at[e])

    @pl.when(is_host)
    def _():
        wait(xout_buf.at[pl.ds(0, half - 1)], xo_send)

    wait(xout_buf.at[pl.ds(0, extra)], xo_recv)
    wait(out_buf.at[others], o_send)
    wait(out_buf, o_recv)


def store_kernel(a_ref, b_ref, o_ref, ot_ref, sems):
    moves = [
        pltpu.make_async_copy(a_ref, o_ref, sems.at[0]),
        pltpu.make_async_copy(b_ref, ot_ref, sems.at[1]),
    ]
    for move in moves:
        move.start()
    for move in moves:
        move.wait()


def exchanged(n, queries, query_tangents, keys, key_tangents, values, value_tangents, selection):
    rows, width = queries.shape
    half, extra, d = n // 2, HEADS - n, HEAD_DIM
    vm = pltpu.VMEM
    dma = pltpu.SemaphoreType.DMA
    reach = 2 * REACH + 1
    bf = jnp.bfloat16
    landed = pl.pallas_call(
        functools.partial(exchange_kernel, n),
        out_shape=[vm((rows, width), bf)] * 2,
        in_specs=[pl.BlockSpec(memory_space=pl.ANY)] * 7,
        out_specs=[pl.BlockSpec(memory_space=vm)] * 2,
        scratch_shapes=[
            vm((n, rows, 2 * d), bf),
            vm((n, rows, 4 * d), bf),
            vm((half, rows, 2 * d), bf),
            vm((n, rows, 4 * d), bf),
            vm((n,) + selection.shape, jnp.int32),
            vm((n, rows, 2 * d), bf),
            vm((half, rows, 2 * d), bf),
            vm((reach, rows, rows), jnp.float32),
            dma, dma, dma, dma, dma((2, extra)), dma((extra,)), dma,
            dma, dma((n,)), dma, dma, dma, dma, dma,
            pltpu.SemaphoreType.REGULAR((2,)),
        ],
        compiler_params=pltpu.CompilerParams(
            collective_id=0, has_side_effects=True, vmem_limit_bytes=67_043_328 - 4 * rows * width - 131_072
        ),
        name="exchange",
    )(queries, query_tangents, keys, key_tangents, values, value_tangents, selection)
    return pl.pallas_call(
        store_kernel,
        out_shape=[jax.ShapeDtypeStruct((rows, width), bf)] * 2,
        in_specs=[pl.BlockSpec(memory_space=vm)] * 2,
        out_specs=[pl.BlockSpec(memory_space=pl.ANY)] * 2,
        scratch_shapes=[dma((2,))],
        name="store",
    )(*[pltpu.with_memory_space_constraint(x, vm) for x in landed])


def solution(mesh):
    n = mesh.shape["ctx"]
    covered = n == 2 * REACH + 2 and n < HEADS and 2 * (HEADS - n) <= n
    placed = (
        P("ctx", "head"),
        P("ctx", "head"),
        P("ctx", "head"),
        P("ctx", "head"),
        P("ctx", "head"),
        P("ctx", "head"),
        P("ctx", None),
    )
    return jax.shard_map(
        functools.partial(exchanged, n) if covered else body,
        mesh=mesh,
        in_specs=placed,
        out_specs=(P("ctx", "head"), P("ctx", "head")),
        check_vma=False,
    )
```
